512 devices in a mesh: rep: 2 (over core), row: 32 (over x_hi, z), col: 8 (over x_lo, y).
Axes of the slice: x: 4 (x_hi: 2, x_lo: 2; x = x_hi * 2 + x_lo), y: 4, z: 16, core: 2. Of those that a mesh axis runs over, the one named last changes fastest.
Arguments:
- sources: float32 [2, 384, 384, 384], P('rep', 'col', 'row'), may hold values from -6 to 6
Outputs:
- potential: float32 [384, 384, 384], P(('rep', 'col'), 'row')
The draws below stay inside these ranges and needn't reach their ends.
All inputs are finite; a program needn't handle non-finite values.
Results may differ from the reference program's by a relative error of at most 0.000096.
Values sent between devices are 32-bit elements; how exact they have to be, the bound alone decides.
No kernel may reach another device: no remote copies, remote signals or barrier semaphores. Data moves between devices by JAX's collectives and lax.ppermute only.
A program may use at most 64 MiB of HBM per device.

```python
import jax
import jax.numpy as jnp

NA = 384
NB = 384
NC = 384


def draw_sources(key, part):
    noise_key = jax.random.fold_in(key, 0)
    return jnp.clip(jax.random.normal(noise_key, (2, NA, NB, NC), jnp.float32), -6.0, 6.0)


def setup_inputs(seed: int = 0) -> dict:
    streams_of = jax.random.split(jax.random.key(seed), 2)
    return {
        "sources": draw_sources(jax.random.fold_in(streams_of[1], 71), 0),
    }


def laplace_eigen(length):
    modes = jnp.arange(length, dtype=jnp.int32).astype(jnp.float32)
    sines = jnp.sin(modes * (jnp.pi / length))
    return 4.0 * sines * sines


def reference(sources):
    density = sources[0] + sources[1]
    spectrum = jnp.fft.fftn(density)
    eigen_a = laplace_eigen(NA)
    eigen_b = laplace_eigen(NB)
    eigen_c = laplace_eigen(NC)
    total = eigen_a[:, None, None] + eigen_b[None, :, None] + eigen_c[None, None, :] + 0.001
    green = 1.0 / total
    potential = jnp.real(jnp.fft.ifftn(spectrum * green))
    return potential.astype(jnp.float32)
```

```python
import numpy as np

import jax
import jax.numpy as jnp
from jax import lax
from jax.sharding import PartitionSpec as P

N = 384
SHIFT = 0.001


def hartley_table():
    turns = np.outer(np.arange(N), np.arange(N)) % N
    angle = turns * (2.0 * np.pi / N)
    return (np.cos(angle) + np.sin(angle)).astype(np.float32)


def eigen_line():
    return (4.0 * np.sin(np.pi * np.arange(N) / N) ** 2).astype(np.float32)


def dot3(a, b, dims):
    return lax.dot_general(a, b, (dims, ((), ())), precision=lax.Precision.HIGH,
                           preferred_element_type=jnp.float32)


def body(sources):
    rep, col, row = lax.axis_index("rep"), lax.axis_index("col"), lax.axis_index("row")
    n_rep, n_col, n_row = lax.axis_size("rep"), lax.axis_size("col"), lax.axis_size("row")
    group = n_rep * n_col
    table = jnp.asarray(hartley_table())
    part = sources[0]
    nb = part.shape[1]
    na = part.shape[0] // n_rep
    ns = N // group
    halves = part.reshape(n_rep, na, nb, N)
    mine = lax.dynamic_index_in_dim(halves, rep, 0, keepdims=False)
    other = lax.dynamic_index_in_dim(halves, 1 - rep, 0, keepdims=False)
    density = mine + lax.ppermute(other, "rep", [(0, 1), (1, 0)])
    modes = dot3(density.reshape(na * nb, N), table, ((1,), (0,)))
    modes = modes.reshape(na, nb, group, ns).transpose(2, 0, 1, 3)
    modes = lax.all_to_all(modes.reshape(group, 1, na * nb * ns), ("rep", "col"), 0, 0, tiled=True)
    lines = modes.reshape(N, nb * ns)
    table_in = table.reshape(n_col, n_rep, na, N).transpose(1, 0, 2, 3).reshape(N, N)
    field = dot3(lines, table_in, ((0,), (0,))).reshape(nb, ns, N)
    eig = jnp.asarray(eigen_line())
    third = lax.dynamic_slice_in_dim(eig, (rep * n_col + col) * ns, ns)
    lam = third[:, None] + eig[None, :] + SHIFT
    root = jnp.sqrt(lam * (lam + 4.0))
    ratio = 2.0 / (2.0 + lam + root)
    powers = [jnp.ones_like(ratio)]
    for _ in range(nb):
        powers.append(powers[-1] * ratio)
    right = field[0]
    for i in range(1, nb):
        right = right * ratio + field[i]
    left = field[nb - 1]
    for i in range(nb - 2, -1, -1):
        left = left * ratio + field[i]
    waves = jnp.stack([right, left]).reshape(n_row, 1, 2 * ns * N // n_row)
    waves = lax.all_to_all(waves, "row", 0, 0, tiled=True)
    step = jnp.broadcast_to(powers[nb], (2, ns, N)).reshape(n_row, 1, 2 * ns * N // n_row)
    step = lax.dynamic_index_in_dim(step, row, 0, keepdims=True)
    per = 2 * ns * N // n_row
    chunks = waves.reshape(n_row, per)
    step = step.reshape(1, per)
    is_right = lax.broadcasted_iota(jnp.int32, (1, per), 1) + row * per < ns * N
    reach = 1
    while reach < n_row:
        back = jnp.roll(chunks, reach, 0)
        ahead = jnp.roll(chunks, -reach, 0)
        chunks = chunks + step * jnp.where(is_right, back, ahead)
        step = step * step
        reach *= 2
    chunks = chunks / (1.0 - step)
    chunks = jnp.where(is_right, jnp.roll(chunks, 1, 0), jnp.roll(chunks, -1, 0))
    waves = lax.all_to_all(chunks.reshape(n_row, 1, per), "row", 0, 0, tiled=True)
    waves = waves.reshape(2, ns, N)
    scale = (1.0 / (N * N)) / root
    run = waves[0]
    forward = []
    for i in range(nb):
        run = run * ratio
        forward.append(run)
        run = run + field[i]
    run = waves[1]
    result = [None] * nb
    for i in range(nb - 1, -1, -1):
        run = run * ratio + field[i]
        result[i] = (forward[i] + run) * scale
    result = jnp.stack(result)
    lines = dot3(table, result.reshape(nb * ns, N), ((0,), (1,)))
    lines = lax.all_to_all(lines.reshape(group, 1, na * nb * ns), ("rep", "col"), 0, 0, tiled=True)
    modes = lines.reshape(group, na, nb, ns).transpose(1, 2, 0, 3).reshape(na * nb, N)
    return dot3(modes, table, ((1,), (0,))).reshape(na, nb, N)


def solution(mesh):
    return jax.shard_map(
        body,
        mesh=mesh,
        in_specs=(P("rep", "col", "row", None),),
        out_specs=P(("rep", "col"), "row", None),
        check_vma=False,
    )
```

```python
import ml_dtypes
import numpy as np

import jax
import jax.numpy as jnp
from jax import lax
from jax.experimental import pallas as pl
from jax.experimental.pallas import tpu as pltpu
from jax.sharding import PartitionSpec as P

N = 384
SHIFT = 0.001
REP, COL, ROW = 2, 8, 32
GROUP = REP * COL
BLOCK = N // GROUP
CELLS = N // ROW
LINES = CELLS * BLOCK
TILES = BLOCK // 8
PACKED = 2 * TILES + 1
F32 = jnp.float32
BF16 = jnp.bfloat16


def block_of(member):
    return member % COL * REP + member // COL


def member_of(block):
    return block % REP * COL + block // REP


def tables():
    order = [
        BLOCK * block_of(member) + 8 * tile + low
        for tile in range(TILES)
        for member in range(GROUP)
        for low in range(8)
    ]
    turns = np.outer(np.asarray(order), np.arange(N)) % N
    angle = turns * (2.0 * np.pi / N)
    cas = np.cos(angle) + np.sin(angle)
    high = cas.astype(ml_dtypes.bfloat16)
    low = (cas - high.astype(np.float64)).astype(ml_dtypes.bfloat16)
    return high, low


def eigen_line():
    return (4.0 * np.sin(np.pi * np.arange(N) / N) ** 2).astype(np.float32)


def halves(x):
    high = x.astype(BF16)
    return high, (x - high.astype(F32)).astype(BF16)


def product(first, second, contract):
    dims = (contract, ((), ()))
    (fh, fl), (sh, sl) = first, second
    out = lax.dot_general(fl, sh, dims, preferred_element_type=F32)
    out += lax.dot_general(fh, sl, dims, preferred_element_type=F32)
    return out + lax.dot_general(fh, sh, dims, preferred_element_type=F32)


def lanes(shape):
    return lax.broadcasted_iota(jnp.int32, shape, 1)


def swapped(parts, width):
    parts = list(parts)
    lane = lanes(parts[0].shape)
    bit = 1
    while bit < len(parts):
        reach = width * bit
        upper = (lane & reach) != 0
        for i in range(len(parts)):
            if i & bit:
                continue
            a, b = parts[i], parts[i | bit]
            parts[i] = jnp.where(upper, pltpu.roll(b, reach, 1), a)
            parts[i | bit] = jnp.where(upper, b, pltpu.roll(a, 128 - reach, 1))
        bit *= 2
    return parts


def send_lines(lines, high_ref, low_ref, out_ref, slot_of):
    pad = jnp.zeros((N - LINES, N), BF16)
    lines = tuple(jnp.concatenate([part, pad], 0) for part in halves(lines))
    got = product((high_ref[...], low_ref[...]), lines, ((1,), (1,)))
    rows = 8 * GROUP
    lane = lanes((rows, 128))
    rest = got[0:rows, 256:384]
    for tile in range(1, TILES):
        moved = pltpu.roll(got[rows * tile : rows * (tile + 1), 256:384], 32 * tile, 1)
        rest = jnp.where(lane < 32 * tile, rest, moved)
    for member in range(GROUP):
        slot = slot_of(member)
        for tile in range(TILES):
            at = rows * tile + 8 * member
            for half in range(2):
                to = 8 * (2 * tile + half)
                out_ref[slot, to : to + 8, :] = got[at : at + 8, 128 * half : 128 * half + 128]
        to = 8 * (PACKED - 1)
        out_ref[slot, to : to + 8, :] = rest[8 * member : 8 * member + 8]


def received_lines(in_ref, lines_ref):
    parts = swapped([in_ref[member] for member in range(GROUP)], 8)
    for unit in range(CELLS * TILES):
        cell, piece = unit // TILES, unit % TILES
        for tile in range(TILES):
            if unit < 32:
                source = parts[unit % 16]
                at = 8 * (2 * tile + unit // 16)
            else:
                source = parts[4 * tile + unit - 32]
                at = 8 * (PACKED - 1)
            to = BLOCK * cell + 8 * tile
            lines_ref[to : to + 8, 128 * piece : 128 * piece + 128] = source[at : at + 8]


def ratio_of(lam):
    root = jnp.sqrt(lam * (lam + 4.0))
    return 2.0 / (2.0 + lam + root), root


def pieces_of(x):
    return [
        x[8 * tile : 8 * tile + 8, 128 * part : 128 * part + 128]
        for tile in range(TILES)
        for part in range(N // 128)
    ]


def first_kernel(mine_ref, got_ref, high_ref, low_ref, out_ref):
    density = (mine_ref[...] + got_ref[...]).reshape(LINES, N)
    send_lines(density, high_ref, low_ref, out_ref, lambda member: member)


def second_kernel(in_ref, lam_ref, high_ref, low_ref, field_ref, waves_ref, step_ref, lines_ref):
    received_lines(in_ref, lines_ref)
    table = (high_ref[...], low_ref[...])
    field_ref[...] = product(halves(lines_ref[...]), table, ((1,), (0,)))
    ratio, _ = ratio_of(lam_ref[...])
    right = field_ref[0:BLOCK, :]
    left = field_ref[LINES - BLOCK : LINES, :]
    for i in range(1, CELLS):
        right = right * ratio + field_ref[BLOCK * i : BLOCK * (i + 1), :]
        j = CELLS - 1 - i
        left = left * ratio + field_ref[BLOCK * j : BLOCK * (j + 1), :]
    square = ratio * ratio
    fourth = square * square
    step = pieces_of(fourth * fourth * fourth)
    right, left = pieces_of(right), pieces_of(left)
    empty = jnp.zeros((8, 128), F32)
    extra = (right[8], left[8], empty, empty)
    parts = swapped(
        [
            jnp.concatenate([right[k], right[4 + k], left[k], left[4 + k], extra[k]], 0)
            for k in range(4)
        ],
        32,
    )
    for quarter in range(4):
        for m in range(5):
            row = parts[quarter][8 * m : 8 * m + 8].reshape(8, 1, 128)
            waves_ref[8 * quarter : 8 * quarter + 8, :, 128 * m : 128 * m + 128] = row
    extra = (step[8], step[8], empty, empty)
    parts = swapped([jnp.concatenate([step[k], step[4 + k], extra[k]], 0) for k in range(4)], 32)
    for quarter in range(4):
        for m in range(3):
            to = 8 * (4 * m + quarter)
            step_ref[to : to + 8, :] = parts[quarter][8 * m : 8 * m + 8]


def ring_kernel(row_ref, in_ref, step_ref, out_ref):
    row = row_ref[0]
    low_lane = lanes((ROW, 128)) < 32
    for m in range(5):
        lane_tile = (0, 1, 0, 1, 2)[m]
        step = step_ref[pl.ds(ROW * lane_tile + row, 1), :]
        chunks = in_ref[:, :, 128 * m : 128 * m + 128].reshape(ROW, 128)

        def moved(x, reach):
            if m < 2:
                return pltpu.roll(x, reach, 0)
            if m < 4:
                return pltpu.roll(x, ROW - reach, 0)
            return jnp.where(low_lane, pltpu.roll(x, reach, 0), pltpu.roll(x, ROW - reach, 0))

        reach = 1
        while reach < ROW:
            chunks = chunks + step * moved(chunks, reach)
            step = step * step
            reach *= 2
        chunks = moved(chunks / (1.0 - step), 1)
        out_ref[:, :, 128 * m : 128 * m + 128] = chunks.reshape(ROW, 1, 128)


def third_kernel(field_ref, in_ref, lam_ref, high_ref, low_ref, out_ref, lines_ref):
    parts = swapped(
        [
            jnp.concatenate(
                [
                    in_ref[8 * quarter : 8 * quarter + 8, :, 128 * m : 128 * m + 128].reshape(8, 128)
                    for m in range(5)
                ],
                0,
            )
            for quarter in range(4)
        ],
        32,
    )

    def joined(first, second, last):
        tiles = [parts[k][8 * first : 8 * first + 8] for k in range(4)]
        tiles += [parts[k][8 * second : 8 * second + 8] for k in range(4)]
        tiles.append(parts[last][32:40])
        return jnp.concatenate([jnp.concatenate(tiles[3 * t : 3 * t + 3], 1) for t in range(3)], 0)

    ratio, root = ratio_of(lam_ref[...])
    scale = (1.0 / (N * N)) / root
    run = joined(0, 1, 0)
    for i in range(CELLS):
        run = run * ratio
        lines_ref[BLOCK * i : BLOCK * (i + 1), :] = run
        run = run + field_ref[BLOCK * i : BLOCK * (i + 1), :]
    run = joined(2, 3, 1)
    for i in range(CELLS - 1, -1, -1):
        at = slice(BLOCK * i, BLOCK * (i + 1))
        run = run * ratio + field_ref[at, :]
        lines_ref[at, :] = (lines_ref[at, :] + run) * scale
    send_lines(lines_ref[...], high_ref, low_ref, out_ref, block_of)


def last_kernel(in_ref, high_ref, low_ref, out_ref, lines_ref):
    received_lines(in_ref, lines_ref)
    table = (high_ref[...], low_ref[...])
    result = product(halves(lines_ref[...]), table, ((1,), (0,)))
    out_ref[...] = result.reshape(CELLS, BLOCK, N)


def shaped(*shape):
    return jax.ShapeDtypeStruct(shape, F32)


def lines_scratch():
    return pltpu.VMEM((LINES, N), F32)


def exchange(x):
    return lax.all_to_all(x, ("rep", "col"), 0, 0, tiled=True)


def body(sources):
    rep, col, row = lax.axis_index("rep"), lax.axis_index("col"), lax.axis_index("row")
    high, low = (jnp.asarray(part) for part in tables())
    part = jnp.transpose(sources[0], (1, 0, 2))
    mine = lax.dynamic_slice_in_dim(part, rep * BLOCK, BLOCK, 1)
    other = lax.dynamic_slice_in_dim(part, (1 - rep) * BLOCK, BLOCK, 1)
    got = lax.ppermute(other, "rep", [(0, 1), (1, 0)])
    eigen = jnp.asarray(eigen_line())
    third = lax.dynamic_slice_in_dim(eigen, (col * REP + rep) * BLOCK, BLOCK)
    lam = third[:, None] + eigen[None, :] + SHIFT
    packed = shaped(GROUP, 8 * PACKED, 128)
    waves = shaped(ROW, 1, 640)
    modes = pl.pallas_call(first_kernel, out_shape=packed, name="first")(mine, got, high, low)
    field, sums, step = pl.pallas_call(
        second_kernel,
        out_shape=(shaped(LINES, N), waves, shaped(3 * ROW, 128)),
        scratch_shapes=[lines_scratch()],
        name="second",
    )(exchange(modes), lam, high, low)
    sums = lax.all_to_all(sums, "row", 0, 0, tiled=True)
    vmem = pl.BlockSpec(memory_space=pltpu.VMEM)
    sums = pl.pallas_call(
        ring_kernel,
        in_specs=[pl.BlockSpec(memory_space=pltpu.SMEM), vmem, vmem],
        out_shape=waves,
        name="ring",
    )(row.reshape(1), sums, step)
    sums = lax.all_to_all(sums, "row", 0, 0, tiled=True)
    lines = pl.pallas_call(
        third_kernel, out_shape=packed, scratch_shapes=[lines_scratch()], name="third"
    )(field, sums, lam, high, low)
    result = pl.pallas_call(
        last_kernel,
        out_shape=shaped(CELLS, BLOCK, N),
        scratch_shapes=[lines_scratch()],
        name="last",
    )(exchange(lines), high, low)
    return jnp.transpose(result, (1, 0, 2))


def solution(mesh):
    return jax.shard_map(
        body,
        mesh=mesh,
        in_specs=(P("rep", "col", "row", None),),
        out_specs=P(("rep", "col"), "row", None),
        check_vma=False,
    )
```

```python
import ml_dtypes
import numpy as np

import jax
import jax.numpy as jnp
from jax import lax
from jax.experimental import pallas as pl
from jax.experimental.pallas import tpu as pltpu
from jax.sharding import PartitionSpec as P

N = 384
SHIFT = 0.001
REP, COL, ROW = 2, 8, 32
GROUP = REP * COL
BLOCK = N // GROUP
CELLS = N // ROW
LINES = CELLS * BLOCK
TILES = BLOCK // 8
PACKED = 2 * TILES + 1
VMEM_BYTES = 12 * 2**20
F32 = jnp.float32
BF16 = jnp.bfloat16


def block_of(member):
    return member % COL * REP + member // COL


def member_of(block):
    return block % REP * COL + block // REP


def tables():
    order = [
        BLOCK * block_of(member) + 8 * tile + low
        for tile in range(TILES)
        for member in range(GROUP)
        for low in range(8)
    ]
    turns = np.outer(np.asarray(order), np.arange(N)) % N
    angle = turns * (2.0 * np.pi / N)
    cas = np.cos(angle) + np.sin(angle)
    high = cas.astype(ml_dtypes.bfloat16)
    low = (cas - high.astype(np.float64)).astype(ml_dtypes.bfloat16)
    return high, low


def eigen_line():
    return (4.0 * np.sin(np.pi * np.arange(N) / N) ** 2).astype(np.float32)


def halves(x):
    high = x.astype(BF16)
    return high, (x - high.astype(F32)).astype(BF16)


def product(first, second, contract):
    dims = (contract, ((), ()))
    (fh, fl), (sh, sl) = first, second
    out = lax.dot_general(fl, sh, dims, preferred_element_type=F32)
    out += lax.dot_general(fh, sl, dims, preferred_element_type=F32)
    return out + lax.dot_general(fh, sh, dims, preferred_element_type=F32)


def lanes(shape):
    return lax.broadcasted_iota(jnp.int32, shape, 1)


def swapped(parts, width):
    parts = list(parts)
    lane = lanes(parts[0].shape)
    bit = 1
    while bit < len(parts):
        reach = width * bit
        upper = (lane & reach) != 0
        for i in range(len(parts)):
            if i & bit:
                continue
            a, b = parts[i], parts[i | bit]
            parts[i] = jnp.where(upper, pltpu.roll(b, reach, 1), a)
            parts[i | bit] = jnp.where(upper, b, pltpu.roll(a, 128 - reach, 1))
        bit *= 2
    return parts


def send_lines(lines, high_ref, low_ref, out_ref, slot_of):
    pad = jnp.zeros((N - LINES, N), BF16)
    lines = tuple(jnp.concatenate([part, pad], 0) for part in halves(lines))
    got = product((high_ref[...], low_ref[...]), lines, ((1,), (1,)))
    rows = 8 * GROUP
    lane = lanes((rows, 128))
    rest = got[0:rows, 256:384]
    for tile in range(1, TILES):
        moved = pltpu.roll(got[rows * tile : rows * (tile + 1), 256:384], 32 * tile, 1)
        rest = jnp.where(lane < 32 * tile, rest, moved)
    for member in range(GROUP):
        slot = slot_of(member)
        for tile in range(TILES):
            at = rows * tile + 8 * member
            for half in range(2):
                to = 8 * (2 * tile + half)
                out_ref[slot, to : to + 8, :] = got[at : at + 8, 128 * half : 128 * half + 128]
        to = 8 * (PACKED - 1)
        out_ref[slot, to : to + 8, :] = rest[8 * member : 8 * member + 8]


def received_lines(in_ref, lines_ref):
    parts = swapped([in_ref[member] for member in range(GROUP)], 8)
    for unit in range(CELLS * TILES):
        cell, piece = unit // TILES, unit % TILES
        for tile in range(TILES):
            if unit < 32:
                source = parts[unit % 16]
                at = 8 * (2 * tile + unit // 16)
            else:
                source = parts[4 * tile + unit - 32]
                at = 8 * (PACKED - 1)
            to = BLOCK * cell + 8 * tile
            lines_ref[to : to + 8, 128 * piece : 128 * piece + 128] = source[at : at + 8]


def ratio_of(lam):
    root = jnp.sqrt(lam * (lam + 4.0))
    return 2.0 / (2.0 + lam + root), root


def pieces_of(x):
    return [
        x[8 * tile : 8 * tile + 8, 128 * part : 128 * part + 128]
        for tile in range(TILES)
        for part in range(N // 128)
    ]


def first_kernel(mine_ref, got_ref, high_ref, low_ref, out_ref):
    density = (mine_ref[...] + got_ref[...]).reshape(LINES, N)
    send_lines(density, high_ref, low_ref, out_ref, lambda member: member)


def second_kernel(in_ref, lam_ref, high_ref, low_ref, field_ref, waves_ref, step_ref, lines_ref):
    received_lines(in_ref, lines_ref)
    table = (high_ref[...], low_ref[...])
    field_ref[...] = product(halves(lines_ref[...]), table, ((1,), (0,)))
    ratio, _ = ratio_of(lam_ref[...])
    right = field_ref[0:BLOCK, :]
    left = field_ref[LINES - BLOCK : LINES, :]
    for i in range(1, CELLS):
        right = right * ratio + field_ref[BLOCK * i : BLOCK * (i + 1), :]
        j = CELLS - 1 - i
        left = left * ratio + field_ref[BLOCK * j : BLOCK * (j + 1), :]
    square = ratio * ratio
    fourth = square * square
    step = pieces_of(fourth * fourth * fourth)
    right, left = pieces_of(right), pieces_of(left)
    empty = jnp.zeros((8, 128), F32)
    extra = (right[8], left[8], empty, empty)
    parts = swapped(
        [
            jnp.concatenate([right[k], right[4 + k], left[k], left[4 + k], extra[k]], 0)
            for k in range(4)
        ],
        32,
    )
    for quarter in range(4):
        for m in range(5):
            row = parts[quarter][8 * m : 8 * m + 8].reshape(8, 1, 128)
            waves_ref[8 * quarter : 8 * quarter + 8, :, 128 * m : 128 * m + 128] = row
    extra = (step[8], step[8], empty, empty)
    parts = swapped([jnp.concatenate([step[k], step[4 + k], extra[k]], 0) for k in range(4)], 32)
    for quarter in range(4):
        for m in range(3):
            to = 8 * (4 * m + quarter)
            step_ref[to : to + 8, :] = parts[quarter][8 * m : 8 * m + 8]


def ring_kernel(row_ref, in_ref, step_ref, out_ref):
    row = row_ref[0]
    low_lane = lanes((ROW, 128)) < 32
    for m in range(5):
        lane_tile = (0, 1, 0, 1, 2)[m]
        step = step_ref[pl.ds(ROW * lane_tile + row, 1), :]
        chunks = in_ref[:, :, 128 * m : 128 * m + 128].reshape(ROW, 128)

        def moved(x, reach):
            if m < 2:
                return pltpu.roll(x, reach, 0)
            if m < 4:
                return pltpu.roll(x, ROW - reach, 0)
            return jnp.where(low_lane, pltpu.roll(x, reach, 0), pltpu.roll(x, ROW - reach, 0))

        reach = 1
        while reach < ROW:
            chunks = chunks + step * moved(chunks, reach)
            step = step * step
            reach *= 2
        chunks = moved(chunks / (1.0 - step), 1)
        out_ref[:, :, 128 * m : 128 * m + 128] = chunks.reshape(ROW, 1, 128)


def third_kernel(field_ref, in_ref, lam_ref, high_ref, low_ref, out_ref, lines_ref):
    parts = swapped(
        [
            jnp.concatenate(
                [
                    in_ref[8 * quarter : 8 * quarter + 8, :, 128 * m : 128 * m + 128].reshape(8, 128)
                    for m in range(5)
                ],
                0,
            )
            for quarter in range(4)
        ],
        32,
    )

    def joined(first, second, last):
        tiles = [parts[k][8 * first : 8 * first + 8] for k in range(4)]
        tiles += [parts[k][8 * second : 8 * second + 8] for k in range(4)]
        tiles.append(parts[last][32:40])
        return jnp.concatenate([jnp.concatenate(tiles[3 * t : 3 * t + 3], 1) for t in range(3)], 0)

    ratio, root = ratio_of(lam_ref[...])
    scale = (1.0 / (N * N)) / root
    run = joined(0, 1, 0)
    for i in range(CELLS):
        run = run * ratio
        lines_ref[BLOCK * i : BLOCK * (i + 1), :] = run
        run = run + field_ref[BLOCK * i : BLOCK * (i + 1), :]
    run = joined(2, 3, 1)
    for i in range(CELLS - 1, -1, -1):
        at = slice(BLOCK * i, BLOCK * (i + 1))
        run = run * ratio + field_ref[at, :]
        lines_ref[at, :] = (lines_ref[at, :] + run) * scale
    send_lines(lines_ref[...], high_ref, low_ref, out_ref, block_of)


def last_kernel(in_ref, high_ref, low_ref, out_ref, lines_ref):
    received_lines(in_ref, lines_ref)
    table = (high_ref[...], low_ref[...])
    result = product(halves(lines_ref[...]), table, ((1,), (0,)))
    out_ref[...] = result.reshape(CELLS, BLOCK, N)


def call(kernel, name, **kwargs):
    params = pltpu.CompilerParams(vmem_limit_bytes=VMEM_BYTES)
    return pl.pallas_call(kernel, name=name, compiler_params=params, **kwargs)


def shaped(*shape):
    return jax.ShapeDtypeStruct(shape, F32)


def lines_scratch():
    return pltpu.VMEM((LINES, N), F32)


def copy_kernel(rep_ref, in_ref, out_ref):
    out_ref[...] = in_ref[...]


def own_half(part, rep):
    shape = (CELLS, BLOCK, N)
    grid_spec = pltpu.PrefetchScalarGridSpec(
        num_scalar_prefetch=1,
        grid=(1,),
        in_specs=[pl.BlockSpec(shape, lambda i, rep_ref: (0, rep_ref[0], 0))],
        out_specs=pl.BlockSpec(shape, lambda i, rep_ref: (0, 0, 0)),
    )
    out = shaped(*shape)
    return call(copy_kernel, "mine", grid_spec=grid_spec, out_shape=out)(rep.reshape(1), part)


def exchange(x):
    return lax.all_to_all(x, ("rep", "col"), 0, 0, tiled=True)


def body(sources):
    rep, col, row = lax.axis_index("rep"), lax.axis_index("col"), lax.axis_index("row")
    high, low = (jnp.asarray(part) for part in tables())
    part = jnp.transpose(sources[0], (1, 0, 2))
    mine = own_half(part, rep)
    other = lax.dynamic_slice_in_dim(part, (1 - rep) * BLOCK, BLOCK, 1)
    got = lax.ppermute(other, "rep", [(0, 1), (1, 0)])
    eigen = jnp.asarray(eigen_line())
    third = lax.dynamic_slice_in_dim(eigen, (col * REP + rep) * BLOCK, BLOCK)
    lam = third[:, None] + eigen[None, :] + SHIFT
    packed = shaped(GROUP, 8 * PACKED, 128)
    waves = shaped(ROW, 1, 640)
    modes = call(first_kernel, "first", out_shape=packed)(mine, got, high, low)
    modes, lam, place = lax.optimization_barrier((modes, lam, row.reshape(1)))
    field, sums, step = call(
        second_kernel,
        "second",
        out_shape=(shaped(LINES, N), waves, shaped(3 * ROW, 128)),
        scratch_shapes=[lines_scratch()],
    )(exchange(modes), lam, high, low)
    sums = lax.all_to_all(sums, "row", 0, 0, tiled=True)
    vmem = pl.BlockSpec(memory_space=pltpu.VMEM)
    sums = call(
        ring_kernel,
        "ring",
        in_specs=[pl.BlockSpec(memory_space=pltpu.SMEM), vmem, vmem],
        out_shape=waves,
    )(place, sums, step)
    sums = lax.all_to_all(sums, "row", 0, 0, tiled=True)
    lines = call(third_kernel, "third", out_shape=packed, scratch_shapes=[lines_scratch()])(
        field, sums, lam, high, low
    )
    result = call(
        last_kernel,
        "last",
        out_shape=shaped(CELLS, BLOCK, N),
        scratch_shapes=[lines_scratch()],
    )(exchange(lines), high, low)
    return jnp.transpose(result, (1, 0, 2))


def solution(mesh):
    return jax.shard_map(
        body,
        mesh=mesh,
        in_specs=(P("rep", "col", "row", None),),
        out_specs=P(("rep", "col"), "row", None),
        check_vma=False,
    )
```

```python
import ml_dtypes
import numpy as np

import jax
import jax.numpy as jnp
from jax import lax
from jax.experimental import pallas as pl
from jax.experimental.pallas import tpu as pltpu
from jax.sharding import PartitionSpec as P

N = 384
SHIFT = 0.001
REP, COL, ROW = 2, 8, 32
ARC = ROW // 2
GROUP = REP * COL
BLOCK = N // GROUP
CELLS = N // ROW
LINES = CELLS * BLOCK
TILES = BLOCK // 8
PACKED = 2 * TILES + 1
WAVES = 9
PARTS = 3
VMEM_BYTES = 12 * 2**20
F32 = jnp.float32
BF16 = jnp.bfloat16


def block_of(member):
    return member % COL * REP + member // COL


def member_of(block):
    return block % REP * COL + block // REP


def tables():
    order = [
        BLOCK * block_of(member) + 8 * tile + low
        for tile in range(TILES)
        for member in range(GROUP)
        for low in range(8)
    ]
    turns = np.outer(np.asarray(order), np.arange(N)) % N
    angle = turns * (2.0 * np.pi / N)
    cas = np.cos(angle) + np.sin(angle)
    high = cas.astype(ml_dtypes.bfloat16)
    low = (cas - high.astype(np.float64)).astype(ml_dtypes.bfloat16)
    return high, low


def eigen_line():
    return (4.0 * np.sin(np.pi * np.arange(N) / N) ** 2).astype(np.float32)


def halves(x):
    high = x.astype(BF16)
    return high, (x - high.astype(F32)).astype(BF16)


def product(first, second, contract):
    dims = (contract, ((), ()))
    (fh, fl), (sh, sl) = first, second
    out = lax.dot_general(fl, sh, dims, preferred_element_type=F32)
    out += lax.dot_general(fh, sl, dims, preferred_element_type=F32)
    return out + lax.dot_general(fh, sh, dims, preferred_element_type=F32)


def lanes(shape):
    return lax.broadcasted_iota(jnp.int32, shape, 1)


def swapped(parts, width):
    parts = list(parts)
    lane = lanes(parts[0].shape)
    bit = 1
    while bit < len(parts):
        reach = width * bit
        upper = (lane & reach) != 0
        for i in range(len(parts)):
            if i & bit:
                continue
            a, b = parts[i], parts[i | bit]
            parts[i] = jnp.where(upper, pltpu.roll(b, reach, 1), a)
            parts[i | bit] = jnp.where(upper, b, pltpu.roll(a, 128 - reach, 1))
        bit *= 2
    return parts


def send_lines(lines, high_ref, low_ref, out_ref, slot_of):
    pad = jnp.zeros((N - LINES, N), BF16)
    lines = tuple(jnp.concatenate([part, pad], 0) for part in halves(lines))
    got = product((high_ref[...], low_ref[...]), lines, ((1,), (1,)))
    rows = 8 * GROUP
    lane = lanes((rows, 128))
    rest = got[0:rows, 256:384]
    for tile in range(1, TILES):
        moved = pltpu.roll(got[rows * tile : rows * (tile + 1), 256:384], 32 * tile, 1)
        rest = jnp.where(lane < 32 * tile, rest, moved)
    for member in range(GROUP):
        slot = slot_of(member)
        for tile in range(TILES):
            at = rows * tile + 8 * member
            for half in range(2):
                to = 8 * (2 * tile + half)
                out_ref[slot, to : to + 8, :] = got[at : at + 8, 128 * half : 128 * half + 128]
        to = 8 * (PACKED - 1)
        out_ref[slot, to : to + 8, :] = rest[8 * member : 8 * member + 8]


def received_lines(in_ref, lines_ref):
    parts = swapped([in_ref[member] for member in range(GROUP)], 8)
    for unit in range(CELLS * TILES):
        cell, piece = unit // TILES, unit % TILES
        for tile in range(TILES):
            if unit < 32:
                source = parts[unit % 16]
                at = 8 * (2 * tile + unit // 16)
            else:
                source = parts[4 * tile + unit - 32]
                at = 8 * (PACKED - 1)
            to = BLOCK * cell + 8 * tile
            lines_ref[to : to + 8, 128 * piece : 128 * piece + 128] = source[at : at + 8]


def ratio_of(lam):
    root = jnp.sqrt(lam * (lam + 4.0))
    return 2.0 / (2.0 + lam + root), root


def pieces_of(x):
    return [
        x[8 * tile : 8 * tile + 8, 128 * part : 128 * part + 128]
        for tile in range(TILES)
        for part in range(N // 128)
    ]


def first_kernel(mine_ref, got_ref, high_ref, low_ref, out_ref):
    density = (mine_ref[...] + got_ref[...]).reshape(LINES, N)
    send_lines(density, high_ref, low_ref, out_ref, lambda member: member)


def second_kernel(in_ref, lam_ref, high_ref, low_ref, field_ref, waves_ref, step_ref, lines_ref):
    received_lines(in_ref, lines_ref)
    table = (high_ref[...], low_ref[...])
    field_ref[...] = product(halves(lines_ref[...]), table, ((1,), (0,)))
    ratio, _ = ratio_of(lam_ref[...])
    right = field_ref[0:BLOCK, :]
    left = field_ref[LINES - BLOCK : LINES, :]
    for i in range(1, CELLS):
        right = right * ratio + field_ref[BLOCK * i : BLOCK * (i + 1), :]
        j = CELLS - 1 - i
        left = left * ratio + field_ref[BLOCK * j : BLOCK * (j + 1), :]
    square = ratio * ratio
    fourth = square * square
    step = pieces_of(fourth * fourth * fourth)
    right, left = pieces_of(right), pieces_of(left)
    sides = []
    for k in range(2):
        rows = [*right[k:8:2], *left[k:8:2], (right, left)[k][8]]
        sides.append(jnp.concatenate(rows, 0))
    for half, side in enumerate(swapped(sides, 64)):
        for m in range(WAVES):
            row = side[8 * m : 8 * m + 8].reshape(8, 1, 128)
            waves_ref[8 * half : 8 * half + 8, :, 128 * m : 128 * m + 128] = row
    sides = [jnp.concatenate([*step[k:8:2], step[8]], 0) for k in range(2)]
    for half, side in enumerate(swapped(sides, 64)):
        for m in range(5):
            to = 8 * (2 * m + half)
            step_ref[to : to + 8, :] = side[8 * m : 8 * m + 8]


def wave_step(step_ref, place, m):
    kind = 4 if m == 8 else m % 4
    return step_ref[pl.ds(ARC * kind + place, 1), :]


def arc_kernel(place_ref, in_ref, step_ref, sums_ref, whole_ref):
    place = place_ref[0]
    chunk = lax.broadcasted_iota(jnp.int32, (ARC, 128), 0)
    is_right = lanes((ARC, 128)) < 64
    for m in range(WAVES):
        step = wave_step(step_ref, place, m)
        sums = in_ref[:, :, 128 * m : 128 * m + 128].reshape(ARC, 128)
        reach = 1
        while reach < ARC:
            back = jnp.where(chunk >= reach, pltpu.roll(sums, reach, 0), 0.0)
            ahead = jnp.where(chunk < ARC - reach, pltpu.roll(sums, ARC - reach, 0), 0.0)
            if m < 4:
                moved = back
            elif m < 8:
                moved = ahead
            else:
                moved = jnp.where(is_right, back, ahead)
            sums = sums + step * moved
            step = step * step
            reach *= 2
        sums_ref[:, 128 * m : 128 * m + 128] = sums
        first, last = sums[0:1], sums[ARC - 1 : ARC]
        if m < 4:
            whole = last
        elif m < 8:
            whole = first
        else:
            whole = jnp.where(is_right[0:1], last, first)
        whole_ref[:, 128 * m : 128 * m + 128] = whole


def ring_kernel(place_ref, sums_ref, whole_ref, other_ref, step_ref, out_ref):
    place = place_ref[0]
    chunk = lax.broadcasted_iota(jnp.int32, (ARC, 128), 0)
    is_right = lanes((ARC, 128)) < 64
    for m in range(WAVES):
        at = slice(128 * m, 128 * m + 128)
        step = wave_step(step_ref, place, m)
        sums = sums_ref[:, at]
        back = jnp.where(chunk >= 1, pltpu.roll(sums, 1, 0), 0.0)
        ahead = jnp.where(chunk < ARC - 1, pltpu.roll(sums, ARC - 1, 0), 0.0)
        if m < 4:
            moved, depth = back, chunk
        elif m < 8:
            moved, depth = ahead, ARC - 1 - chunk
        else:
            moved = jnp.where(is_right, back, ahead)
            depth = jnp.where(is_right, chunk, ARC - 1 - chunk)
        decay = jnp.ones((ARC, 128), F32)
        reach = 1
        while reach < ARC:
            decay = jnp.where((depth & reach) != 0, decay * step, decay)
            step = step * step
            reach *= 2
        inflow = (other_ref[:, at] + step * whole_ref[:, at]) / (1.0 - step * step)
        out_ref[:, :, at] = (moved + decay * inflow).reshape(ARC, 1, 128)


def third_kernel(field_ref, in_ref, lam_ref, high_ref, low_ref, out_ref, lines_ref):
    sides = []
    for half in range(2):
        rows = [
            in_ref[8 * half : 8 * half + 8, :, 128 * m : 128 * m + 128].reshape(8, 128)
            for m in range(WAVES)
        ]
        sides.append(jnp.concatenate(rows, 0))
    sides = swapped(sides, 64)

    def joined(start, last):
        tiles = [
            sides[k % 2][8 * (start + k // 2) : 8 * (start + k // 2) + 8] for k in range(8)
        ]
        tiles.append(sides[last][64:72])
        return jnp.concatenate([jnp.concatenate(tiles[3 * t : 3 * t + 3], 1) for t in range(3)], 0)

    ratio, root = ratio_of(lam_ref[...])
    scale = (1.0 / (N * N)) / root
    run = joined(0, 0)
    for i in range(CELLS):
        run = run * ratio
        lines_ref[BLOCK * i : BLOCK * (i + 1), :] = run
        run = run + field_ref[BLOCK * i : BLOCK * (i + 1), :]
    run = joined(4, 1)
    for i in range(CELLS - 1, -1, -1):
        at = slice(BLOCK * i, BLOCK * (i + 1))
        run = run * ratio + field_ref[at, :]
        lines_ref[at, :] = (lines_ref[at, :] + run) * scale
    send_lines(lines_ref[...], high_ref, low_ref, out_ref, block_of)


def last_kernel(in_ref, high_ref, low_ref, out_ref, lines_ref, result_ref, sems):
    received_lines(in_ref, lines_ref)
    table = (high_ref[...], low_ref[...])
    cells = CELLS // PARTS
    copies = []
    for part in range(PARTS):
        rows = halves(lines_ref[BLOCK * cells * part : BLOCK * cells * (part + 1), :])
        result = product(rows, table, ((1,), (0,)))
        at = pl.ds(cells * part, cells)
        result_ref[at] = result.reshape(cells, BLOCK, N)
        copies.append(pltpu.make_async_copy(result_ref.at[at], out_ref.at[at], sems.at[part]))
        copies[-1].start()
    for copy in copies:
        copy.wait()


def call(kernel, name, **kwargs):
    params = pltpu.CompilerParams(vmem_limit_bytes=VMEM_BYTES)
    return pl.pallas_call(kernel, name=name, compiler_params=params, **kwargs)


def shaped(*shape):
    return jax.ShapeDtypeStruct(shape, F32)


def lines_scratch():
    return pltpu.VMEM((LINES, N), F32)


def copy_kernel(rep_ref, in_ref, out_ref):
    out_ref[...] = in_ref[...]


def own_half(part, rep):
    shape = (CELLS, BLOCK, N)
    grid_spec = pltpu.PrefetchScalarGridSpec(
        num_scalar_prefetch=1,
        grid=(1,),
        in_specs=[pl.BlockSpec(shape, lambda i, rep_ref: (0, rep_ref[0], 0))],
        out_specs=pl.BlockSpec(shape, lambda i, rep_ref: (0, 0, 0)),
    )
    out = shaped(*shape)
    return call(copy_kernel, "mine", grid_spec=grid_spec, out_shape=out)(rep.reshape(1), part)


def exchange(x):
    return lax.all_to_all(x, ("rep", "col"), 0, 0, tiled=True)


def arc_exchange(x):
    arcs = [list(range(ARC)), list(range(ARC, ROW))]
    return lax.all_to_all(x, "row", 0, 0, axis_index_groups=arcs, tiled=True)


def body(sources):
    rep, col, row = lax.axis_index("rep"), lax.axis_index("col"), lax.axis_index("row")
    high, low = (jnp.asarray(part) for part in tables())
    part = jnp.transpose(sources[0], (1, 0, 2))
    mine = own_half(part, rep)
    other = lax.dynamic_slice_in_dim(part, (1 - rep) * BLOCK, BLOCK, 1)
    got = lax.ppermute(other, "rep", [(0, 1), (1, 0)])
    eigen = jnp.asarray(eigen_line())
    third = lax.dynamic_slice_in_dim(eigen, (col * REP + rep) * BLOCK, BLOCK)
    lam = third[:, None] + eigen[None, :] + SHIFT
    packed = shaped(GROUP, 8 * PACKED, 128)
    waves = shaped(ARC, 1, 128 * WAVES)
    modes = call(first_kernel, "first", out_shape=packed)(mine, got, high, low)
    place = (row % ARC).reshape(1)
    modes, lam, place = lax.optimization_barrier((modes, lam, place))
    field, sums, step = call(
        second_kernel,
        "second",
        out_shape=(shaped(LINES, N), waves, shaped(5 * ARC, 128)),
        scratch_shapes=[lines_scratch()],
    )(exchange(modes), lam, high, low)
    vmem = pl.BlockSpec(memory_space=pltpu.VMEM)
    smem = pl.BlockSpec(memory_space=pltpu.SMEM)
    sums, whole = call(
        arc_kernel,
        "arc",
        in_specs=[smem, vmem, vmem],
        out_shape=(shaped(ARC, 128 * WAVES), shaped(1, 128 * WAVES)),
    )(place, arc_exchange(sums), step)
    other = lax.ppermute(whole, "row", [(i, (i + ARC) % ROW) for i in range(ROW)])
    sums = call(
        ring_kernel,
        "ring",
        in_specs=[smem, vmem, vmem, vmem, vmem],
        out_shape=waves,
    )(place, sums, whole, other, step)
    sums = arc_exchange(sums)
    lines = call(third_kernel, "third", out_shape=packed, scratch_shapes=[lines_scratch()])(
        field, sums, lam, high, low
    )
    result = call(
        last_kernel,
        "last",
        in_specs=[vmem, vmem, vmem],
        out_specs=pl.BlockSpec(memory_space=pl.ANY),
        out_shape=shaped(CELLS, BLOCK, N),
        scratch_shapes=[
            lines_scratch(),
            pltpu.VMEM((CELLS, BLOCK, N), F32),
            pltpu.SemaphoreType.DMA((PARTS,)),
        ],
    )(exchange(lines), high, low)
    return jnp.transpose(result, (1, 0, 2))


def solution(mesh):
    return jax.shard_map(
        body,
        mesh=mesh,
        in_specs=(P("rep", "col", "row", None),),
        out_specs=P(("rep", "col"), "row", None),
        check_vma=False,
    )
```

```python
import ml_dtypes
import numpy as np

import jax
import jax.numpy as jnp
from jax import lax
from jax.experimental import pallas as pl
from jax.experimental.pallas import tpu as pltpu
from jax.sharding import Mesh
from jax.sharding import PartitionSpec as P

N = 384
SHIFT = 0.001
REP, COL, ROW = 2, 8, 32
GROUP = REP * COL
BLOCK = N // GROUP
CELLS = N // ROW
LINES = CELLS * BLOCK
TILES = BLOCK // 8
PACKED = 2 * TILES + 1
PARTS, PAIR = 4, 2
RING = ROW // PARTS
VMEM_BYTES = 12 * 2**20
F32 = jnp.float32
BF16 = jnp.bfloat16


def block_of(member):
    return member % COL * REP + member // COL


def member_of(block):
    return block % REP * COL + block // REP


def tables():
    order = [
        BLOCK * block_of(member) + 8 * tile + low
        for tile in range(TILES)
        for member in range(GROUP)
        for low in range(8)
    ]
    turns = np.outer(np.asarray(order), np.arange(N)) % N
    angle = turns * (2.0 * np.pi / N)
    cas = np.cos(angle) + np.sin(angle)
    high = cas.astype(ml_dtypes.bfloat16)
    low = (cas - high.astype(np.float64)).astype(ml_dtypes.bfloat16)
    return high, low


def eigen_line():
    return (4.0 * np.sin(np.pi * np.arange(N) / N) ** 2).astype(np.float32)


def halves(x):
    high = x.astype(BF16)
    return high, (x - high.astype(F32)).astype(BF16)


def product(first, second, contract):
    dims = (contract, ((), ()))
    (fh, fl), (sh, sl) = first, second
    out = lax.dot_general(fl, sh, dims, preferred_element_type=F32)
    out += lax.dot_general(fh, sl, dims, preferred_element_type=F32)
    return out + lax.dot_general(fh, sh, dims, preferred_element_type=F32)


def lanes(shape):
    return lax.broadcasted_iota(jnp.int32, shape, 1)


def swapped(parts, width):
    parts = list(parts)
    lane = lanes(parts[0].shape)
    bit = 1
    while bit < len(parts):
        reach = width * bit
        upper = (lane & reach) != 0
        for i in range(len(parts)):
            if i & bit:
                continue
            a, b = parts[i], parts[i | bit]
            parts[i] = jnp.where(upper, pltpu.roll(b, reach, 1), a)
            parts[i | bit] = jnp.where(upper, b, pltpu.roll(a, 128 - reach, 1))
        bit *= 2
    return parts


def ratio_of(lam):
    root = jnp.sqrt(lam * (lam + 4.0))
    return 2.0 / (2.0 + lam + root), root


def send_tile(out_ref, member, piece, tile):
    for part in range(PARTS):
        out_ref[PARTS * member + part, piece] = tile[PAIR * part : PAIR * (part + 1), :]


def received(in_ref, member):
    parts = [in_ref[PARTS * member + part] for part in range(PARTS)]
    return jnp.concatenate(parts, 1).reshape(8 * PACKED, 128)


def unit_place(unit, tile):
    if unit < 32:
        return unit % 16, 8 * (2 * tile + unit // 16)
    return 4 * tile + unit - 32, 8 * (PACKED - 1)


def first_kernel(mine_ref, got_ref, high_ref, low_ref, out_ref):
    density = (mine_ref[...] + got_ref[...]).reshape(LINES, N)
    pad = jnp.zeros((N - LINES, N), BF16)
    lines = tuple(jnp.concatenate([part, pad], 0) for part in halves(density))
    modes = product((high_ref[...], low_ref[...]), lines, ((1,), (1,)))
    rows = 8 * GROUP
    lane = lanes((rows, 128))
    rest = modes[0:rows, 256:384]
    for tile in range(1, TILES):
        moved = pltpu.roll(modes[rows * tile : rows * (tile + 1), 256:384], 32 * tile, 1)
        rest = jnp.where(lane < 32 * tile, rest, moved)
    for member in range(GROUP):
        at = 8 * member
        for tile in range(TILES):
            row = rows * tile + at
            for half in range(2):
                piece = modes[row : row + 8, 128 * half : 128 * half + 128]
                send_tile(out_ref, member, 2 * tile + half, piece)
        send_tile(out_ref, member, PACKED - 1, rest[at : at + 8])


def second_kernel(
    in_ref, lam_ref, high_ref, low_ref, field_ref, right_ref, left_ref, waves_ref, lines_ref
):
    packed = swapped([received(in_ref, member) for member in range(GROUP)], 8)
    for unit in range(CELLS * TILES):
        cell, piece = unit // TILES, unit % TILES
        for tile in range(TILES):
            source, at = unit_place(unit, tile)
            to = BLOCK * cell + 8 * tile
            lanes_to = slice(128 * piece, 128 * piece + 128)
            lines_ref[to : to + 8, lanes_to] = packed[source][at : at + 8]
    table = (high_ref[...], low_ref[...])
    field_ref[...] = product(halves(lines_ref[...]), table, ((1,), (0,)))
    ratio, _ = ratio_of(lam_ref[...])
    right = field_ref[0:BLOCK, :]
    left = field_ref[LINES - BLOCK : LINES, :]
    for i in range(1, CELLS):
        right = right * ratio + field_ref[BLOCK * i : BLOCK * (i + 1), :]
        j = CELLS - 1 - i
        left = left * ratio + field_ref[BLOCK * j : BLOCK * (j + 1), :]
    right_ref[...] = right
    left_ref[...] = left
    step = chunk_step(ratio)
    lower = sublanes((8, N)) < 4
    for tile in range(TILES):
        at = slice(8 * tile, 8 * tile + 8)
        joined = jnp.where(
            lower,
            step[at] * right[at] + pltpu.roll(right[at], 4, 0),
            step[at] * left[at] + pltpu.roll(left[at], 4, 0),
        )
        for member in range(RING):
            waves_ref[member, at, :] = joined


def chunk_step(ratio):
    square = ratio * ratio
    fourth = square * square
    return fourth * fourth * fourth


def sublanes(shape):
    return lax.broadcasted_iota(jnp.int32, shape, 0)


def ring_inflow(place, waves_ref, at, step):
    pair = step * step
    zero = jnp.zeros((8, N), F32)
    sides = []
    for forward in (True, False):
        before, rest, whole, decay = zero, zero, zero, jnp.ones((8, N), F32)
        for k in range(RING):
            member = k if forward else RING - 1 - k
            wave = waves_ref[member, at, :]
            earlier = member < place if forward else member > place
            before = jnp.where(earlier, before * pair + wave, before)
            rest = jnp.where(earlier, rest, rest * pair + wave)
            whole = whole * pair + wave
            decay = jnp.where(earlier, decay * pair, decay)
        sides.append((before, rest, whole, decay))
    row = sublanes((8, N))
    before, rest, whole, decay = (jnp.where(row < 4, *both) for both in zip(*sides))
    first_arc = (row & 2) == 0
    other = jnp.where(first_arc, pltpu.roll(whole, 6, 0), pltpu.roll(whole, 2, 0))
    power = pair
    for _ in range(3):
        power = power * power
    return (before + decay * (other + power * rest)) / (1.0 - power * power)


def third_kernel(
    place_ref,
    field_ref,
    right_ref,
    left_ref,
    waves_ref,
    lam_ref,
    high_ref,
    low_ref,
    out_ref,
    lines_ref,
):
    ratio, root = ratio_of(lam_ref[...])
    step = chunk_step(ratio)
    lower = sublanes((8, N)) < 4
    forward, backward = [], []
    for tile in range(TILES):
        at = slice(8 * tile, 8 * tile + 8)
        inflow = ring_inflow(place_ref[0], waves_ref, at, step[at])
        turned = pltpu.roll(inflow, 4, 0)
        right = pltpu.roll(right_ref[at, :], 4, 0)
        left = pltpu.roll(left_ref[at, :], 4, 0)
        forward.append(jnp.where(lower, inflow, step[at] * turned + right))
        backward.append(jnp.where(lower, step[at] * turned + left, inflow))
    scale = (1.0 / (N * N)) / root
    run = jnp.concatenate(forward, 0)
    for i in range(CELLS):
        run = run * ratio
        lines_ref[BLOCK * i : BLOCK * (i + 1), :] = run
        run = run + field_ref[BLOCK * i : BLOCK * (i + 1), :]
    run = jnp.concatenate(backward, 0)
    for i in range(CELLS - 1, -1, -1):
        at = slice(BLOCK * i, BLOCK * (i + 1))
        run = run * ratio + field_ref[at, :]
        lines_ref[at, :] = (lines_ref[at, :] + run) * scale
    table = (high_ref[...], low_ref[...])
    lines_ref[...] = product(halves(lines_ref[...]), table, ((1,), (1,)))
    tiles = [[jnp.zeros((8, 128), F32)] * PACKED for _ in range(GROUP)]
    for unit in range(CELLS * TILES):
        cell, piece = unit // TILES, unit % TILES
        for tile in range(TILES):
            source, at = unit_place(unit, tile)
            row = BLOCK * cell + 8 * tile
            tiles[source][at // 8] = lines_ref[row : row + 8, 128 * piece : 128 * piece + 128]
    packed = swapped([jnp.concatenate(group, 0) for group in tiles], 8)
    for member in range(GROUP):
        slot = block_of(member)
        for piece in range(PACKED):
            send_tile(out_ref, slot, piece, packed[member][8 * piece : 8 * piece + 8])


def last_kernel(in_ref, high_ref, low_ref, out_ref, modes_ref):
    for member in range(GROUP):
        packed = received(in_ref, member)
        rest = packed[8 * (PACKED - 1) : 8 * PACKED]
        for tile in range(TILES):
            row = 8 * (GROUP * tile + member)
            for half in range(2):
                at = 8 * (2 * tile + half)
                modes_ref[row : row + 8, 128 * half : 128 * half + 128] = packed[at : at + 8]
            moved = rest if tile == 0 else pltpu.roll(rest, 128 - 32 * tile, 1)
            modes_ref[row : row + 8, 256:384] = moved
    table = (high_ref[...], low_ref[...])
    result = product(halves(modes_ref[...].T[0:LINES]), table, ((1,), (0,)))
    out_ref[...] = result.reshape(CELLS, BLOCK, N)


def call(kernel, name, **kwargs):
    params = pltpu.CompilerParams(vmem_limit_bytes=VMEM_BYTES)
    return pl.pallas_call(kernel, name=name, compiler_params=params, **kwargs)


def shaped(*shape):
    return jax.ShapeDtypeStruct(shape, F32)


def lines_scratch():
    return pltpu.VMEM((LINES, N), F32)


def copy_kernel(rep_ref, in_ref, out_ref):
    out_ref[...] = in_ref[...]


def own_half(part, rep):
    shape = (CELLS, BLOCK, N)
    grid_spec = pltpu.PrefetchScalarGridSpec(
        num_scalar_prefetch=1,
        grid=(1,),
        in_specs=[pl.BlockSpec(shape, lambda i, rep_ref: (0, rep_ref[0], 0))],
        out_specs=pl.BlockSpec(shape, lambda i, rep_ref: (0, 0, 0)),
    )
    out = shaped(*shape)
    return call(copy_kernel, "mine", grid_spec=grid_spec, out_shape=out)(rep.reshape(1), part)


def exchange(x):
    return lax.all_to_all(x, ("rep", "col", "zl", "xh"), 0, 0, tiled=True)


def body(sources):
    rep, col = lax.axis_index("rep"), lax.axis_index("col")
    part_index = lax.axis_index("zl") * 2 + lax.axis_index("xh")
    high, low = (jnp.asarray(part) for part in tables())
    part = jnp.transpose(sources[0], (1, 0, 2))
    mine = own_half(part, rep)
    other = lax.dynamic_slice_in_dim(part, (1 - rep) * BLOCK, BLOCK, 1)
    got = lax.ppermute(other, "rep", [(0, 1), (1, 0)])
    eigen = jnp.asarray(eigen_line())
    third = lax.dynamic_slice_in_dim(eigen, (col * REP + rep) * BLOCK, BLOCK)
    third = lax.dynamic_index_in_dim(third.reshape(TILES, PARTS, PAIR), part_index, 1)
    third = jnp.broadcast_to(third, (TILES, PARTS, PAIR)).reshape(BLOCK)
    lam = third[:, None] + eigen[None, :] + SHIFT
    packed = shaped(GROUP * PARTS, PACKED, PAIR, 128)
    modes = call(first_kernel, "first", out_shape=packed)(mine, got, high, low)
    place = lax.axis_index("zh").reshape(1)
    modes, lam, place = lax.optimization_barrier((modes, lam, place))
    side = shaped(BLOCK, N)
    field, right, left, waves = call(
        second_kernel,
        "second",
        out_shape=(shaped(LINES, N), side, side, shaped(RING, BLOCK, N)),
        scratch_shapes=[lines_scratch()],
    )(exchange(modes), lam, high, low)
    waves = lax.all_to_all(waves, "zh", 0, 0, tiled=True)
    vmem = pl.BlockSpec(memory_space=pltpu.VMEM)
    lines = call(
        third_kernel,
        "third",
        in_specs=[pl.BlockSpec(memory_space=pltpu.SMEM)] + [vmem] * 7,
        out_shape=packed,
        scratch_shapes=[lines_scratch()],
    )(place, field, right, left, waves, lam, high, low)
    result = call(
        last_kernel,
        "last",
        out_shape=shaped(CELLS, BLOCK, N),
        scratch_shapes=[pltpu.VMEM((N, N), F32)],
    )(exchange(lines), high, low)
    return jnp.transpose(result, (1, 0, 2))


def solution(mesh):
    devices = mesh.devices.reshape(REP, 2, RING, 2, COL)
    split = Mesh(devices, ("rep", "xh", "zh", "zl", "col"))
    row = ("xh", "zh", "zl")
    return jax.shard_map(
        body,
        mesh=split,
        in_specs=(P("rep", "col", row, None),),
        out_specs=P(("rep", "col"), row, None),
        check_vma=False,
    )
```

```python
import ml_dtypes
import numpy as np

import jax
import jax.numpy as jnp
from jax import lax
from jax.experimental import pallas as pl
from jax.experimental.pallas import tpu as pltpu
from jax.sharding import Mesh
from jax.sharding import PartitionSpec as P

N = 384
SHIFT = 0.001
REP, COL, ROW = 2, 8, 32
GROUP = REP * COL
BLOCK = N // GROUP
CELLS = N // ROW
LINES = CELLS * BLOCK
TILES = BLOCK // 8
PACKED = 2 * TILES + 1
PARTS, PAIR = 4, 2
RING = ROW // PARTS
VMEM_BYTES = 12 * 2**20
F32 = jnp.float32
BF16 = jnp.bfloat16


def member_at(rep, col):
    return col % 4 * 4 + rep * 2 + col // 4


def block_of(member):
    rep, col = member // 2 % 2, member % 2 * 4 + member // 4
    return col * REP + rep


def tables():
    order = [
        BLOCK * block_of(member) + 8 * tile + low
        for tile in range(TILES)
        for member in range(GROUP)
        for low in range(8)
    ]
    turns = np.outer(np.asarray(order), np.arange(N)) % N
    angle = turns * (2.0 * np.pi / N)
    cas = np.cos(angle) + np.sin(angle)
    high = cas.astype(ml_dtypes.bfloat16)
    low = (cas - high.astype(np.float64)).astype(ml_dtypes.bfloat16)
    return high, low


def eigen_line():
    return (4.0 * np.sin(np.pi * np.arange(N) / N) ** 2).astype(np.float32)


def third_eigen():
    rows = [
        [
            BLOCK * block_of(member) + 8 * tile + PAIR * part + low
            for tile in range(TILES)
            for _ in range(PARTS)
            for low in range(PAIR)
        ]
        for member in range(GROUP)
        for part in range(PARTS)
    ]
    return eigen_line()[np.asarray(rows)]


def halves(x):
    high = x.astype(BF16)
    return high, (x - high.astype(F32)).astype(BF16)


def product(first, second, contract):
    dims = (contract, ((), ()))
    (fh, fl), (sh, sl) = first, second
    out = lax.dot_general(fl, sh, dims, preferred_element_type=F32)
    out += lax.dot_general(fh, sl, dims, preferred_element_type=F32)
    return out + lax.dot_general(fh, sh, dims, preferred_element_type=F32)


def lanes(shape):
    return lax.broadcasted_iota(jnp.int32, shape, 1)


def swapped(parts, width):
    parts = list(parts)
    lane = lanes(parts[0].shape)
    bit = 1
    while bit < len(parts):
        reach = width * bit
        upper = (lane & reach) != 0
        for i in range(len(parts)):
            if i & bit:
                continue
            a, b = parts[i], parts[i | bit]
            parts[i] = jnp.where(upper, pltpu.roll(b, reach, 1), a)
            parts[i | bit] = jnp.where(upper, b, pltpu.roll(a, 128 - reach, 1))
        bit *= 2
    return parts


def ratio_of(lam):
    root = jnp.sqrt(lam * (lam + 4.0))
    return 2.0 / (2.0 + lam + root), root


def send_tile(out_ref, member, piece, tile, twist=0):
    for part in range(PARTS):
        slot = GROUP * (part ^ twist) + member
        out_ref[slot, piece] = tile[PAIR * part : PAIR * (part + 1), :]


def received(in_ref, member, twist=0):
    parts = [in_ref[GROUP * (part ^ twist) + member] for part in range(PARTS)]
    return jnp.concatenate(parts, 1).reshape(8 * PACKED, 128)


def unit_place(unit, tile):
    if unit < 32:
        return unit % 16, 8 * (2 * tile + unit // 16)
    return 4 * tile + unit - 32, 8 * (PACKED - 1)


def first_kernel(twist_ref, mine_ref, got_ref, high_ref, low_ref, out_ref):
    density = (mine_ref[...] + got_ref[...]).reshape(LINES, N)
    pad = jnp.zeros((N - LINES, N), BF16)
    lines = tuple(jnp.concatenate([part, pad], 0) for part in halves(density))
    modes = product((high_ref[...], low_ref[...]), lines, ((1,), (1,)))
    rows = 8 * GROUP
    lane = lanes((rows, 128))
    rest = modes[0:rows, 256:384]
    for tile in range(1, TILES):
        moved = pltpu.roll(modes[rows * tile : rows * (tile + 1), 256:384], 32 * tile, 1)
        rest = jnp.where(lane < 32 * tile, rest, moved)
    for member in range(GROUP):
        at = 8 * member
        for tile in range(TILES):
            row = rows * tile + at
            for half in range(2):
                piece = modes[row : row + 8, 128 * half : 128 * half + 128]
                send_tile(out_ref, member, 2 * tile + half, piece, twist_ref[0])
        send_tile(out_ref, member, PACKED - 1, rest[at : at + 8], twist_ref[0])


def second_kernel(
    in_ref, lam_ref, high_ref, low_ref, field_ref, right_ref, left_ref, waves_ref, lines_ref
):
    packed = swapped([received(in_ref, member) for member in range(GROUP)], 8)
    for unit in range(CELLS * TILES):
        cell, piece = unit // TILES, unit % TILES
        for tile in range(TILES):
            source, at = unit_place(unit, tile)
            to = BLOCK * cell + 8 * tile
            lanes_to = slice(128 * piece, 128 * piece + 128)
            lines_ref[to : to + 8, lanes_to] = packed[source][at : at + 8]
    table = (high_ref[...], low_ref[...])
    field_ref[...] = product(halves(lines_ref[...]), table, ((1,), (0,)))
    ratio, _ = ratio_of(lam_ref[...])
    right = field_ref[0:BLOCK, :]
    left = field_ref[LINES - BLOCK : LINES, :]
    for i in range(1, CELLS):
        right = right * ratio + field_ref[BLOCK * i : BLOCK * (i + 1), :]
        j = CELLS - 1 - i
        left = left * ratio + field_ref[BLOCK * j : BLOCK * (j + 1), :]
    right_ref[...] = right
    left_ref[...] = left
    step = chunk_step(ratio)
    lower = sublanes((8, N)) < 4
    for tile in range(TILES):
        at = slice(8 * tile, 8 * tile + 8)
        joined = jnp.where(
            lower,
            step[at] * right[at] + pltpu.roll(right[at], 4, 0),
            step[at] * left[at] + pltpu.roll(left[at], 4, 0),
        )
        for member in range(RING):
            waves_ref[member, at, :] = joined


def chunk_step(ratio):
    square = ratio * ratio
    fourth = square * square
    return fourth * fourth * fourth


def sublanes(shape):
    return lax.broadcasted_iota(jnp.int32, shape, 0)


def ring_inflow(place, waves_ref, at, step):
    pair = step * step
    zero = jnp.zeros((8, N), F32)
    sides = []
    for forward in (True, False):
        before, rest, whole, decay = zero, zero, zero, jnp.ones((8, N), F32)
        for k in range(RING):
            member = k if forward else RING - 1 - k
            wave = waves_ref[member, at, :]
            earlier = member < place if forward else member > place
            before = jnp.where(earlier, before * pair + wave, before)
            rest = jnp.where(earlier, rest, rest * pair + wave)
            whole = whole * pair + wave
            decay = jnp.where(earlier, decay * pair, decay)
        sides.append((before, rest, whole, decay))
    row = sublanes((8, N))
    before, rest, whole, decay = (jnp.where(row < 4, *both) for both in zip(*sides))
    first_arc = (row & 2) == 0
    other = jnp.where(first_arc, pltpu.roll(whole, 6, 0), pltpu.roll(whole, 2, 0))
    power = pair
    for _ in range(3):
        power = power * power
    return (before + decay * (other + power * rest)) / (1.0 - power * power)


def third_kernel(
    place_ref,
    field_ref,
    right_ref,
    left_ref,
    waves_ref,
    lam_ref,
    high_ref,
    low_ref,
    out_ref,
    lines_ref,
):
    ratio, root = ratio_of(lam_ref[...])
    step = chunk_step(ratio)
    lower = sublanes((8, N)) < 4
    forward, backward = [], []
    for tile in range(TILES):
        at = slice(8 * tile, 8 * tile + 8)
        inflow = ring_inflow(place_ref[0], waves_ref, at, step[at])
        turned = pltpu.roll(inflow, 4, 0)
        right = pltpu.roll(right_ref[at, :], 4, 0)
        left = pltpu.roll(left_ref[at, :], 4, 0)
        forward.append(jnp.where(lower, inflow, step[at] * turned + right))
        backward.append(jnp.where(lower, step[at] * turned + left, inflow))
    scale = (1.0 / (N * N)) / root
    run = jnp.concatenate(forward, 0)
    for i in range(CELLS):
        run = run * ratio
        lines_ref[BLOCK * i : BLOCK * (i + 1), :] = run
        run = run + field_ref[BLOCK * i : BLOCK * (i + 1), :]
    run = jnp.concatenate(backward, 0)
    for i in range(CELLS - 1, -1, -1):
        at = slice(BLOCK * i, BLOCK * (i + 1))
        run = run * ratio + field_ref[at, :]
        lines_ref[at, :] = (lines_ref[at, :] + run) * scale
    table = (high_ref[...], low_ref[...])
    lines_ref[...] = product(halves(lines_ref[...]), table, ((1,), (1,)))
    tiles = [[jnp.zeros((8, 128), F32)] * PACKED for _ in range(GROUP)]
    for unit in range(CELLS * TILES):
        cell, piece = unit // TILES, unit % TILES
        for tile in range(TILES):
            source, at = unit_place(unit, tile)
            row = BLOCK * cell + 8 * tile
            tiles[source][at // 8] = lines_ref[row : row + 8, 128 * piece : 128 * piece + 128]
    packed = swapped([jnp.concatenate(group, 0) for group in tiles], 8)
    for member in range(GROUP):
        slot = member_at(*divmod(block_of(member), COL))
        for piece in range(PACKED):
            send_tile(out_ref, slot, piece, packed[member][8 * piece : 8 * piece + 8])


def last_kernel(twist_ref, in_ref, high_ref, low_ref, out_ref, modes_ref):
    for member in range(GROUP):
        packed = received(in_ref, member, twist_ref[0])
        rest = packed[8 * (PACKED - 1) : 8 * PACKED]
        for tile in range(TILES):
            row = 8 * (GROUP * tile + member)
            for half in range(2):
                at = 8 * (2 * tile + half)
                modes_ref[row : row + 8, 128 * half : 128 * half + 128] = packed[at : at + 8]
            moved = rest if tile == 0 else pltpu.roll(rest, 128 - 32 * tile, 1)
            modes_ref[row : row + 8, 256:384] = moved
    table = (high_ref[...], low_ref[...])
    result = product(halves(modes_ref[...].T[0:LINES]), table, ((1,), (0,)))
    out_ref[...] = result.reshape(CELLS, BLOCK, N)


def call(kernel, name, **kwargs):
    params = pltpu.CompilerParams(vmem_limit_bytes=VMEM_BYTES)
    return pl.pallas_call(kernel, name=name, compiler_params=params, **kwargs)


def shaped(*shape):
    return jax.ShapeDtypeStruct(shape, F32)


def lines_scratch():
    return pltpu.VMEM((LINES, N), F32)


def copy_kernel(rep_ref, in_ref, out_ref):
    out_ref[...] = in_ref[...]


def own_half(part, rep):
    shape = (CELLS, BLOCK, N)
    grid_spec = pltpu.PrefetchScalarGridSpec(
        num_scalar_prefetch=1,
        grid=(1,),
        in_specs=[pl.BlockSpec(shape, lambda i, rep_ref: (0, rep_ref[0], 0))],
        out_specs=pl.BlockSpec(shape, lambda i, rep_ref: (0, 0, 0)),
    )
    out = shaped(*shape)
    return call(copy_kernel, "mine", grid_spec=grid_spec, out_shape=out)(rep.reshape(1), part)


def exchange(x):
    return lax.all_to_all(x, ("zl", "xh", "y", "rep", "xl"), 0, 0, tiled=True)


def ring_exchange(x):
    rings = [[2 * k + (half ^ (k // (RING // 2))) for k in range(RING)] for half in range(2)]
    return lax.all_to_all(x, ("zh", "zl"), 0, 0, axis_index_groups=rings, tiled=True)


def body(sources):
    rep, col = lax.axis_index("rep"), lax.axis_index("xl") * 4 + lax.axis_index("y")
    place = lax.axis_index("zh")
    twist = 2 * (place // (RING // 2))
    part_index = (lax.axis_index("zl") * 2 + lax.axis_index("xh")) ^ twist
    high, low = (jnp.asarray(part) for part in tables())
    part = jnp.transpose(sources[0], (1, 0, 2))
    mine = own_half(part, rep)
    other = lax.dynamic_slice_in_dim(part, (1 - rep) * BLOCK, BLOCK, 1)
    got = lax.ppermute(other, "rep", [(0, 1), (1, 0)])
    eigen = jnp.asarray(eigen_line())
    third = jnp.asarray(third_eigen())
    third = lax.dynamic_index_in_dim(third, member_at(rep, col) * PARTS + part_index, keepdims=False)
    lam = third[:, None] + eigen[None, :] + SHIFT
    packed = shaped(GROUP * PARTS, PACKED, PAIR, 128)
    vmem = pl.BlockSpec(memory_space=pltpu.VMEM)
    smem = pl.BlockSpec(memory_space=pltpu.SMEM)
    place, twist = place.reshape(1), twist.reshape(1)
    modes = call(first_kernel, "first", in_specs=[smem] + [vmem] * 4, out_shape=packed)(
        twist, mine, got, high, low
    )
    modes, lam, place, twist = lax.optimization_barrier((modes, lam, place, twist))
    side = shaped(BLOCK, N)
    field, right, left, waves = call(
        second_kernel,
        "second",
        out_shape=(shaped(LINES, N), side, side, shaped(RING, BLOCK, N)),
        scratch_shapes=[lines_scratch()],
    )(exchange(modes), lam, high, low)
    waves = ring_exchange(waves)
    lines = call(
        third_kernel,
        "third",
        in_specs=[smem] + [vmem] * 7,
        out_shape=packed,
        scratch_shapes=[lines_scratch()],
    )(place, field, right, left, waves, lam, high, low)
    result = call(
        last_kernel,
        "last",
        in_specs=[smem] + [vmem] * 3,
        out_shape=shaped(CELLS, BLOCK, N),
        scratch_shapes=[pltpu.VMEM((N, N), F32)],
    )(twist, exchange(lines), high, low)
    return jnp.transpose(result, (1, 0, 2))


def solution(mesh):
    devices = mesh.devices.reshape(REP, 2, RING, 2, 2, 4)
    split = Mesh(devices, ("rep", "xh", "zh", "zl", "xl", "y"))
    row, col = ("xh", "zh", "zl"), ("xl", "y")
    return jax.shard_map(
        body,
        mesh=split,
        in_specs=(P("rep", col, row, None),),
        out_specs=P(("rep", *col), row, None),
        check_vma=False,
    )
```

```python
import ml_dtypes
import numpy as np

import jax
import jax.numpy as jnp
from jax import lax
from jax.experimental import pallas as pl
from jax.experimental.pallas import tpu as pltpu
from jax.sharding import Mesh
from jax.sharding import PartitionSpec as P

N = 384
SHIFT = 0.001
REP, COL, ROW = 2, 8, 32
GROUP = REP * COL
BLOCK = N // GROUP
CELLS = N // ROW
LINES = CELLS * BLOCK
TILES = BLOCK // 8
PACKED = 2 * TILES + 1
PARTS, PAIR = 4, 2
RING = ROW // PARTS
ORDER = (4, 0, 5, 1, 6, 2, 7, 3)
VMEM_BYTES = 12 * 2**20
F32 = jnp.float32
BF16 = jnp.bfloat16


def member_at(rep, col):
    return col % 4 * 4 + rep * 2 + col // 4


def block_of(member):
    rep, col = member // 2 % 2, member % 2 * 4 + member // 4
    return col * REP + rep


def tables():
    order = [
        BLOCK * block_of(member) + 8 * tile + low
        for tile in range(TILES)
        for member in range(GROUP)
        for low in range(8)
    ]
    turns = np.outer(np.asarray(order), np.arange(N)) % N
    angle = turns * (2.0 * np.pi / N)
    cas = np.cos(angle) + np.sin(angle)
    high = cas.astype(ml_dtypes.bfloat16)
    low = (cas - high.astype(np.float64)).astype(ml_dtypes.bfloat16)
    return high, low


def eigen_line():
    return (4.0 * np.sin(np.pi * np.arange(N) / N) ** 2).astype(np.float32)


def third_eigen():
    rows = [
        [
            BLOCK * block_of(member) + 8 * tile + PAIR * part + low
            for tile in range(TILES)
            for _ in range(PARTS)
            for low in range(PAIR)
        ]
        for member in range(GROUP)
        for part in range(PARTS)
    ]
    return eigen_line()[np.asarray(rows)]


def halves(x):
    high = x.astype(BF16)
    return high, (x - high.astype(F32)).astype(BF16)


def product(first, second, contract):
    dims = (contract, ((), ()))
    (fh, fl), (sh, sl) = first, second
    out = lax.dot_general(fl, sh, dims, preferred_element_type=F32)
    out += lax.dot_general(fh, sl, dims, preferred_element_type=F32)
    return out + lax.dot_general(fh, sh, dims, preferred_element_type=F32)


def lanes(shape):
    return lax.broadcasted_iota(jnp.int32, shape, 1)


def swapped(parts, width):
    parts = list(parts)
    lane = lanes(parts[0].shape)
    bit = 1
    while bit < len(parts):
        reach = width * bit
        upper = (lane & reach) != 0
        for i in range(len(parts)):
            if i & bit:
                continue
            a, b = parts[i], parts[i | bit]
            parts[i] = jnp.where(upper, pltpu.roll(b, reach, 1), a)
            parts[i | bit] = jnp.where(upper, b, pltpu.roll(a, 128 - reach, 1))
        bit *= 2
    return parts


def ratio_of(lam):
    root = jnp.sqrt(lam * (lam + 4.0))
    return 2.0 / (2.0 + lam + root), root


def send_tile(out_ref, member, piece, tile, twist=0):
    for part in range(PARTS):
        slot = GROUP * (part ^ twist) + member
        out_ref[slot, piece] = tile[PAIR * part : PAIR * (part + 1), :]


def received(in_ref, member, twist=0):
    parts = [in_ref[GROUP * (part ^ twist) + member] for part in range(PARTS)]
    return jnp.concatenate(parts, 1).reshape(8 * PACKED, 128)


def unit_place(unit, tile):
    if unit < 32:
        return unit % 16, 8 * (2 * tile + unit // 16)
    return 4 * tile + unit - 32, 8 * (PACKED - 1)


def first_kernel(twist_ref, mine_ref, got_ref, high_ref, low_ref, out_ref):
    density = (mine_ref[...] + got_ref[...]).reshape(LINES, N)
    pad = jnp.zeros((N - LINES, N), BF16)
    lines = tuple(jnp.concatenate([part, pad], 0) for part in halves(density))
    modes = product((high_ref[...], low_ref[...]), lines, ((1,), (1,)))
    rows = 8 * GROUP
    lane = lanes((rows, 128))
    rest = modes[0:rows, 256:384]
    for tile in range(1, TILES):
        moved = pltpu.roll(modes[rows * tile : rows * (tile + 1), 256:384], 32 * tile, 1)
        rest = jnp.where(lane < 32 * tile, rest, moved)
    for member in range(GROUP):
        at = 8 * member
        for tile in range(TILES):
            row = rows * tile + at
            for half in range(2):
                piece = modes[row : row + 8, 128 * half : 128 * half + 128]
                send_tile(out_ref, member, 2 * tile + half, piece, twist_ref[0])
        send_tile(out_ref, member, PACKED - 1, rest[at : at + 8], twist_ref[0])


def second_kernel(
    in_ref, lam_ref, high_ref, low_ref, field_ref, right_ref, left_ref, waves_ref, lines_ref
):
    packed = swapped([received(in_ref, member) for member in range(GROUP)], 8)
    for unit in range(CELLS * TILES):
        cell, piece = unit // TILES, unit % TILES
        for tile in range(TILES):
            source, at = unit_place(unit, tile)
            to = BLOCK * cell + 8 * tile
            lanes_to = slice(128 * piece, 128 * piece + 128)
            lines_ref[to : to + 8, lanes_to] = packed[source][at : at + 8]
    table = (high_ref[...], low_ref[...])
    field_ref[...] = product(halves(lines_ref[...]), table, ((1,), (0,)))
    ratio, _ = ratio_of(lam_ref[...])
    right = field_ref[0:BLOCK, :]
    left = field_ref[LINES - BLOCK : LINES, :]
    for i in range(1, CELLS):
        right = right * ratio + field_ref[BLOCK * i : BLOCK * (i + 1), :]
        j = CELLS - 1 - i
        left = left * ratio + field_ref[BLOCK * j : BLOCK * (j + 1), :]
    right_ref[...] = right
    left_ref[...] = left
    step = chunk_step(ratio)
    lower = sublanes((8, N)) < 4
    for tile in range(TILES):
        at = slice(8 * tile, 8 * tile + 8)
        joined = jnp.where(
            lower,
            step[at] * right[at] + pltpu.roll(right[at], 4, 0),
            step[at] * left[at] + pltpu.roll(left[at], 4, 0),
        )
        for member in range(RING):
            waves_ref[member, at, :] = joined


def chunk_step(ratio):
    square = ratio * ratio
    fourth = square * square
    return fourth * fourth * fourth


def sublanes(shape):
    return lax.broadcasted_iota(jnp.int32, shape, 0)


def ring_inflow(place, waves_ref, at, step):
    pair = step * step
    zero = jnp.zeros((8, N), F32)
    sides = []
    for forward in (True, False):
        before, rest, whole, decay = zero, zero, zero, jnp.ones((8, N), F32)
        for k in range(RING):
            member = k if forward else RING - 1 - k
            wave = waves_ref[ORDER.index(member), at, :]
            earlier = member < place if forward else member > place
            before = jnp.where(earlier, before * pair + wave, before)
            rest = jnp.where(earlier, rest, rest * pair + wave)
            whole = whole * pair + wave
            decay = jnp.where(earlier, decay * pair, decay)
        sides.append((before, rest, whole, decay))
    row = sublanes((8, N))
    before, rest, whole, decay = (jnp.where(row < 4, *both) for both in zip(*sides))
    first_arc = (row & 2) == 0
    other = jnp.where(first_arc, pltpu.roll(whole, 6, 0), pltpu.roll(whole, 2, 0))
    power = pair
    for _ in range(3):
        power = power * power
    return (before + decay * (other + power * rest)) / (1.0 - power * power)


def third_kernel(
    place_ref,
    field_ref,
    right_ref,
    left_ref,
    waves_ref,
    lam_ref,
    high_ref,
    low_ref,
    out_ref,
    lines_ref,
):
    ratio, root = ratio_of(lam_ref[...])
    step = chunk_step(ratio)
    lower = sublanes((8, N)) < 4
    forward, backward = [], []
    for tile in range(TILES):
        at = slice(8 * tile, 8 * tile + 8)
        inflow = ring_inflow(place_ref[0], waves_ref, at, step[at])
        turned = pltpu.roll(inflow, 4, 0)
        right = pltpu.roll(right_ref[at, :], 4, 0)
        left = pltpu.roll(left_ref[at, :], 4, 0)
        forward.append(jnp.where(lower, inflow, step[at] * turned + right))
        backward.append(jnp.where(lower, step[at] * turned + left, inflow))
    scale = (1.0 / (N * N)) / root
    run = jnp.concatenate(forward, 0)
    for i in range(CELLS):
        run = run * ratio
        lines_ref[BLOCK * i : BLOCK * (i + 1), :] = run
        run = run + field_ref[BLOCK * i : BLOCK * (i + 1), :]
    run = jnp.concatenate(backward, 0)
    for i in range(CELLS - 1, -1, -1):
        at = slice(BLOCK * i, BLOCK * (i + 1))
        run = run * ratio + field_ref[at, :]
        lines_ref[at, :] = (lines_ref[at, :] + run) * scale
    table = (high_ref[...], low_ref[...])
    lines_ref[...] = product(halves(lines_ref[...]), table, ((1,), (1,)))
    tiles = [[jnp.zeros((8, 128), F32)] * PACKED for _ in range(GROUP)]
    for unit in range(CELLS * TILES):
        cell, piece = unit // TILES, unit % TILES
        for tile in range(TILES):
            source, at = unit_place(unit, tile)
            row = BLOCK * cell + 8 * tile
            tiles[source][at // 8] = lines_ref[row : row + 8, 128 * piece : 128 * piece + 128]
    packed = swapped([jnp.concatenate(group, 0) for group in tiles], 8)
    for member in range(GROUP):
        slot = member_at(*divmod(block_of(member), COL))
        for piece in range(PACKED):
            send_tile(out_ref, slot, piece, packed[member][8 * piece : 8 * piece + 8])


def last_kernel(twist_ref, in_ref, high_ref, low_ref, out_ref, modes_ref):
    for member in range(GROUP):
        packed = received(in_ref, member, twist_ref[0])
        rest = packed[8 * (PACKED - 1) : 8 * PACKED]
        for tile in range(TILES):
            row = 8 * (GROUP * tile + member)
            for half in range(2):
                at = 8 * (2 * tile + half)
                modes_ref[row : row + 8, 128 * half : 128 * half + 128] = packed[at : at + 8]
            moved = rest if tile == 0 else pltpu.roll(rest, 128 - 32 * tile, 1)
            modes_ref[row : row + 8, 256:384] = moved
    table = (high_ref[...], low_ref[...])
    result = product(halves(modes_ref[...].T[0:LINES]), table, ((1,), (0,)))
    out_ref[...] = result.reshape(CELLS, BLOCK, N)


def call(kernel, name, **kwargs):
    params = pltpu.CompilerParams(vmem_limit_bytes=VMEM_BYTES)
    return pl.pallas_call(kernel, name=name, compiler_params=params, **kwargs)


def shaped(*shape):
    return jax.ShapeDtypeStruct(shape, F32)


def lines_scratch():
    return pltpu.VMEM((LINES, N), F32)


def copy_kernel(rep_ref, in_ref, out_ref):
    out_ref[...] = in_ref[...]


def own_half(part, rep):
    shape = (CELLS, BLOCK, N)
    grid_spec = pltpu.PrefetchScalarGridSpec(
        num_scalar_prefetch=1,
        grid=(1,),
        in_specs=[pl.BlockSpec(shape, lambda i, rep_ref: (0, rep_ref[0], 0))],
        out_specs=pl.BlockSpec(shape, lambda i, rep_ref: (0, 0, 0)),
    )
    out = shaped(*shape)
    return call(copy_kernel, "mine", grid_spec=grid_spec, out_shape=out)(rep.reshape(1), part)


def exchange(x):
    return lax.all_to_all(x, ("zl", "xh", "y", "rep", "xl"), 0, 0, tiled=True)


def ring_exchange(x):
    rings = [[2 * k + (half ^ (k // (RING // 2))) for k in ORDER] for half in range(2)]
    return lax.all_to_all(x, ("zh", "zl"), 0, 0, axis_index_groups=rings, tiled=True)


def body(sources):
    rep, col = lax.axis_index("rep"), lax.axis_index("xl") * 4 + lax.axis_index("y")
    place = lax.axis_index("zh")
    twist = 2 * (place // (RING // 2))
    part_index = (lax.axis_index("zl") * 2 + lax.axis_index("xh")) ^ twist
    high, low = (jnp.asarray(part) for part in tables())
    part = jnp.transpose(sources[0], (1, 0, 2))
    mine = own_half(part, rep)
    other = lax.dynamic_slice_in_dim(part, (1 - rep) * BLOCK, BLOCK, 1)
    got = lax.ppermute(other, "rep", [(0, 1), (1, 0)])
    eigen = jnp.asarray(eigen_line())
    third = jnp.asarray(third_eigen())
    third = lax.dynamic_index_in_dim(third, member_at(rep, col) * PARTS + part_index, keepdims=False)
    lam = third[:, None] + eigen[None, :] + SHIFT
    packed = shaped(GROUP * PARTS, PACKED, PAIR, 128)
    vmem = pl.BlockSpec(memory_space=pltpu.VMEM)
    smem = pl.BlockSpec(memory_space=pltpu.SMEM)
    place, twist = place.reshape(1), twist.reshape(1)
    modes = call(first_kernel, "first", in_specs=[smem] + [vmem] * 4, out_shape=packed)(
        twist, mine, got, high, low
    )
    modes, lam, place, twist = lax.optimization_barrier((modes, lam, place, twist))
    side = shaped(BLOCK, N)
    field, right, left, waves = call(
        second_kernel,
        "second",
        out_shape=(shaped(LINES, N), side, side, shaped(RING, BLOCK, N)),
        scratch_shapes=[lines_scratch()],
    )(exchange(modes), lam, high, low)
    waves = ring_exchange(waves)
    lines = call(
        third_kernel,
        "third",
        in_specs=[smem] + [vmem] * 7,
        out_shape=packed,
        scratch_shapes=[lines_scratch()],
    )(place, field, right, left, waves, lam, high, low)
    result = call(
        last_kernel,
        "last",
        in_specs=[smem] + [vmem] * 3,
        out_shape=shaped(CELLS, BLOCK, N),
        scratch_shapes=[pltpu.VMEM((N, N), F32)],
    )(twist, exchange(lines), high, low)
    return jnp.transpose(result, (1, 0, 2))


def solution(mesh):
    devices = mesh.devices.reshape(REP, 2, RING, 2, 2, 4)
    split = Mesh(devices, ("rep", "xh", "zh", "zl", "xl", "y"))
    row, col = ("xh", "zh", "zl"), ("xl", "y")
    return jax.shard_map(
        body,
        mesh=split,
        in_specs=(P("rep", col, row, None),),
        out_specs=P(("rep", *col), row, None),
        check_vma=False,
    )
```

```python
import ml_dtypes
import numpy as np

import jax
import jax.numpy as jnp
from jax import lax
from jax.experimental import pallas as pl
from jax.experimental.pallas import tpu as pltpu
from jax.sharding import Mesh
from jax.sharding import PartitionSpec as P

N = 384
SHIFT = 0.001
REP, COL, ROW = 2, 8, 32
GROUP = REP * COL
BLOCK = N // GROUP
CELLS = N // ROW
LINES = CELLS * BLOCK
TILES = BLOCK // 8
PACKED = 2 * TILES + 1
PARTS, PAIR = 4, 2
RING = ROW // PARTS
ORDER = (4, 1, 5, 0, 6, 2, 3, 7)
VMEM_BYTES = 12 * 2**20
F32 = jnp.float32
BF16 = jnp.bfloat16


def member_at(rep, col):
    return col % 4 * 4 + rep * 2 + col // 4


def block_of(member):
    rep, col = member // 2 % 2, member % 2 * 4 + member // 4
    return col * REP + rep


def tables():
    order = [
        BLOCK * block_of(member) + 8 * tile + low
        for tile in range(TILES)
        for member in range(GROUP)
        for low in range(8)
    ]
    turns = np.outer(np.asarray(order), np.arange(N)) % N
    angle = turns * (2.0 * np.pi / N)
    cas = np.cos(angle) + np.sin(angle)
    high = cas.astype(ml_dtypes.bfloat16)
    low = (cas - high.astype(np.float64)).astype(ml_dtypes.bfloat16)
    return high, low


def eigen_line():
    return (4.0 * np.sin(np.pi * np.arange(N) / N) ** 2).astype(np.float32)


def third_eigen():
    rows = [
        [
            BLOCK * block_of(member) + 8 * tile + PAIR * part + low
            for tile in range(TILES)
            for _ in range(PARTS)
            for low in range(PAIR)
        ]
        for member in range(GROUP)
        for part in range(PARTS)
    ]
    return eigen_line()[np.asarray(rows)]


def halves(x):
    high = x.astype(BF16)
    return high, (x - high.astype(F32)).astype(BF16)


def product(first, second, contract):
    dims = (contract, ((), ()))
    (fh, fl), (sh, sl) = first, second
    out = lax.dot_general(fl, sh, dims, preferred_element_type=F32)
    out += lax.dot_general(fh, sl, dims, preferred_element_type=F32)
    return out + lax.dot_general(fh, sh, dims, preferred_element_type=F32)


def lanes(shape):
    return lax.broadcasted_iota(jnp.int32, shape, 1)


def swapped(parts, width):
    parts = list(parts)
    lane = lanes(parts[0].shape)
    bit = 1
    while bit < len(parts):
        reach = width * bit
        upper = (lane & reach) != 0
        for i in range(len(parts)):
            if i & bit:
                continue
            a, b = parts[i], parts[i | bit]
            parts[i] = jnp.where(upper, pltpu.roll(b, reach, 1), a)
            parts[i | bit] = jnp.where(upper, b, pltpu.roll(a, 128 - reach, 1))
        bit *= 2
    return parts


def ratio_of(lam):
    root = jnp.sqrt(lam * (lam + 4.0))
    return 2.0 / (2.0 + lam + root), root


def send_tile(out_ref, member, piece, tile, twist=0):
    for part in range(PARTS):
        slot = GROUP * (part ^ twist) + member
        out_ref[slot, piece] = tile[PAIR * part : PAIR * (part + 1), :]


def received(in_ref, member, twist=0):
    parts = [in_ref[GROUP * (part ^ twist) + member] for part in range(PARTS)]
    return jnp.concatenate(parts, 1).reshape(8 * PACKED, 128)


def unit_place(unit, tile):
    if unit < 32:
        return unit % 16, 8 * (2 * tile + unit // 16)
    return 4 * tile + unit - 32, 8 * (PACKED - 1)


def first_kernel(twist_ref, mine_ref, got_ref, high_ref, low_ref, out_ref):
    density = (mine_ref[...] + got_ref[...]).reshape(LINES, N)
    pad = jnp.zeros((N - LINES, N), BF16)
    lines = tuple(jnp.concatenate([part, pad], 0) for part in halves(density))
    modes = product((high_ref[...], low_ref[...]), lines, ((1,), (1,)))
    rows = 8 * GROUP
    lane = lanes((rows, 128))
    rest = modes[0:rows, 256:384]
    for tile in range(1, TILES):
        moved = pltpu.roll(modes[rows * tile : rows * (tile + 1), 256:384], 32 * tile, 1)
        rest = jnp.where(lane < 32 * tile, rest, moved)
    for member in range(GROUP):
        at = 8 * member
        for tile in range(TILES):
            row = rows * tile + at
            for half in range(2):
                piece = modes[row : row + 8, 128 * half : 128 * half + 128]
                send_tile(out_ref, member, 2 * tile + half, piece, twist_ref[0])
        send_tile(out_ref, member, PACKED - 1, rest[at : at + 8], twist_ref[0])


def second_kernel(
    in_ref, lam_ref, high_ref, low_ref, field_ref, right_ref, left_ref, waves_ref, lines_ref
):
    packed = swapped([received(in_ref, member) for member in range(GROUP)], 8)
    for unit in range(CELLS * TILES):
        cell, piece = unit // TILES, unit % TILES
        for tile in range(TILES):
            source, at = unit_place(unit, tile)
            to = BLOCK * cell + 8 * tile
            lanes_to = slice(128 * piece, 128 * piece + 128)
            lines_ref[to : to + 8, lanes_to] = packed[source][at : at + 8]
    table = (high_ref[...], low_ref[...])
    field_ref[...] = product(halves(lines_ref[...]), table, ((1,), (0,)))
    ratio, _ = ratio_of(lam_ref[...])
    right = field_ref[0:BLOCK, :]
    left = field_ref[LINES - BLOCK : LINES, :]
    for i in range(1, CELLS):
        right = right * ratio + field_ref[BLOCK * i : BLOCK * (i + 1), :]
        j = CELLS - 1 - i
        left = left * ratio + field_ref[BLOCK * j : BLOCK * (j + 1), :]
    right_ref[...] = right
    left_ref[...] = left
    step = chunk_step(ratio)
    lower = sublanes((8, N)) < 4
    for tile in range(TILES):
        at = slice(8 * tile, 8 * tile + 8)
        joined = jnp.where(
            lower,
            step[at] * right[at] + pltpu.roll(right[at], 4, 0),
            step[at] * left[at] + pltpu.roll(left[at], 4, 0),
        )
        for member in range(RING):
            waves_ref[member, at, :] = joined


def chunk_step(ratio):
    square = ratio * ratio
    fourth = square * square
    return fourth * fourth * fourth


def sublanes(shape):
    return lax.broadcasted_iota(jnp.int32, shape, 0)


def ring_inflow(place, waves_ref, at, step):
    pair = step * step
    zero = jnp.zeros((8, N), F32)
    sides = []
    for forward in (True, False):
        before, rest, whole, decay = zero, zero, zero, jnp.ones((8, N), F32)
        for k in range(RING):
            member = k if forward else RING - 1 - k
            wave = waves_ref[ORDER.index(member), at, :]
            earlier = member < place if forward else member > place
            before = jnp.where(earlier, before * pair + wave, before)
            rest = jnp.where(earlier, rest, rest * pair + wave)
            whole = whole * pair + wave
            decay = jnp.where(earlier, decay * pair, decay)
        sides.append((before, rest, whole, decay))
    row = sublanes((8, N))
    before, rest, whole, decay = (jnp.where(row < 4, *both) for both in zip(*sides))
    first_arc = (row & 2) == 0
    other = jnp.where(first_arc, pltpu.roll(whole, 6, 0), pltpu.roll(whole, 2, 0))
    power = pair
    for _ in range(3):
        power = power * power
    return (before + decay * (other + power * rest)) / (1.0 - power * power)


def third_kernel(
    place_ref,
    field_ref,
    right_ref,
    left_ref,
    waves_ref,
    lam_ref,
    high_ref,
    low_ref,
    out_ref,
    lines_ref,
):
    ratio, root = ratio_of(lam_ref[...])
    step = chunk_step(ratio)
    lower = sublanes((8, N)) < 4
    forward, backward = [], []
    for tile in range(TILES):
        at = slice(8 * tile, 8 * tile + 8)
        inflow = ring_inflow(place_ref[0], waves_ref, at, step[at])
        turned = pltpu.roll(inflow, 4, 0)
        right = pltpu.roll(right_ref[at, :], 4, 0)
        left = pltpu.roll(left_ref[at, :], 4, 0)
        forward.append(jnp.where(lower, inflow, step[at] * turned + right))
        backward.append(jnp.where(lower, step[at] * turned + left, inflow))
    scale = (1.0 / (N * N)) / root
    run = jnp.concatenate(forward, 0)
    for i in range(CELLS):
        run = run * ratio
        lines_ref[BLOCK * i : BLOCK * (i + 1), :] = run
        run = run + field_ref[BLOCK * i : BLOCK * (i + 1), :]
    run = jnp.concatenate(backward, 0)
    for i in range(CELLS - 1, -1, -1):
        at = slice(BLOCK * i, BLOCK * (i + 1))
        run = run * ratio + field_ref[at, :]
        lines_ref[at, :] = (lines_ref[at, :] + run) * scale
    table = (high_ref[...], low_ref[...])
    lines_ref[...] = product(halves(lines_ref[...]), table, ((1,), (1,)))
    tiles = [[jnp.zeros((8, 128), F32)] * PACKED for _ in range(GROUP)]
    for unit in range(CELLS * TILES):
        cell, piece = unit // TILES, unit % TILES
        for tile in range(TILES):
            source, at = unit_place(unit, tile)
            row = BLOCK * cell + 8 * tile
            tiles[source][at // 8] = lines_ref[row : row + 8, 128 * piece : 128 * piece + 128]
    packed = swapped([jnp.concatenate(group, 0) for group in tiles], 8)
    for member in range(GROUP):
        slot = member_at(*divmod(block_of(member), COL))
        for piece in range(PACKED):
            send_tile(out_ref, slot, piece, packed[member][8 * piece : 8 * piece + 8])


def last_kernel(twist_ref, in_ref, high_ref, low_ref, out_ref, modes_ref):
    for member in range(GROUP):
        packed = received(in_ref, member, twist_ref[0])
        rest = packed[8 * (PACKED - 1) : 8 * PACKED]
        for tile in range(TILES):
            row = 8 * (GROUP * tile + member)
            for half in range(2):
                at = 8 * (2 * tile + half)
                modes_ref[row : row + 8, 128 * half : 128 * half + 128] = packed[at : at + 8]
            moved = rest if tile == 0 else pltpu.roll(rest, 128 - 32 * tile, 1)
            modes_ref[row : row + 8, 256:384] = moved
    table = (high_ref[...], low_ref[...])
    result = product(halves(modes_ref[...].T[0:LINES]), table, ((1,), (0,)))
    out_ref[...] = result.reshape(CELLS, BLOCK, N)


def call(kernel, name, **kwargs):
    params = pltpu.CompilerParams(vmem_limit_bytes=VMEM_BYTES)
    return pl.pallas_call(kernel, name=name, compiler_params=params, **kwargs)


def shaped(*shape):
    return jax.ShapeDtypeStruct(shape, F32)


def lines_scratch():
    return pltpu.VMEM((LINES, N), F32)


def copy_kernel(rep_ref, in_ref, out_ref):
    out_ref[...] = in_ref[...]


def own_half(part, rep):
    shape = (CELLS, BLOCK, N)
    grid_spec = pltpu.PrefetchScalarGridSpec(
        num_scalar_prefetch=1,
        grid=(1,),
        in_specs=[pl.BlockSpec(shape, lambda i, rep_ref: (0, rep_ref[0], 0))],
        out_specs=pl.BlockSpec(shape, lambda i, rep_ref: (0, 0, 0)),
    )
    out = shaped(*shape)
    return call(copy_kernel, "mine", grid_spec=grid_spec, out_shape=out)(rep.reshape(1), part)


def exchange(x):
    return lax.all_to_all(x, ("zl", "xh", "y", "rep", "xl"), 0, 0, tiled=True)


def ring_exchange(x):
    rings = [[2 * k + (half ^ (k // (RING // 2))) for k in ORDER] for half in range(2)]
    return lax.all_to_all(x, ("zh", "zl"), 0, 0, axis_index_groups=rings, tiled=True)


def body(sources):
    rep, col = lax.axis_index("rep"), lax.axis_index("xl") * 4 + lax.axis_index("y")
    place = lax.axis_index("zh")
    twist = 2 * (place // (RING // 2))
    part_index = (lax.axis_index("zl") * 2 + lax.axis_index("xh")) ^ twist
    high, low = (jnp.asarray(part) for part in tables())
    part = jnp.transpose(sources[0], (1, 0, 2))
    mine = own_half(part, rep)
    other = lax.dynamic_slice_in_dim(part, (1 - rep) * BLOCK, BLOCK, 1)
    got = lax.ppermute(other, "rep", [(0, 1), (1, 0)])
    eigen = jnp.asarray(eigen_line())
    third = jnp.asarray(third_eigen())
    third = lax.dynamic_index_in_dim(third, member_at(rep, col) * PARTS + part_index, keepdims=False)
    lam = third[:, None] + eigen[None, :] + SHIFT
    packed = shaped(GROUP * PARTS, PACKED, PAIR, 128)
    vmem = pl.BlockSpec(memory_space=pltpu.VMEM)
    smem = pl.BlockSpec(memory_space=pltpu.SMEM)
    place, twist = place.reshape(1), twist.reshape(1)
    modes = call(first_kernel, "first", in_specs=[smem] + [vmem] * 4, out_shape=packed)(
        twist, mine, got, high, low
    )
    modes, lam, place, twist = lax.optimization_barrier((modes, lam, place, twist))
    side = shaped(BLOCK, N)
    field, right, left, waves = call(
        second_kernel,
        "second",
        out_shape=(shaped(LINES, N), side, side, shaped(RING, BLOCK, N)),
        scratch_shapes=[lines_scratch()],
    )(exchange(modes), lam, high, low)
    waves = ring_exchange(waves)
    lines = call(
        third_kernel,
        "third",
        in_specs=[smem] + [vmem] * 7,
        out_shape=packed,
        scratch_shapes=[lines_scratch()],
    )(place, field, right, left, waves, lam, high, low)
    result = call(
        last_kernel,
        "last",
        in_specs=[smem] + [vmem] * 3,
        out_shape=shaped(CELLS, BLOCK, N),
        scratch_shapes=[pltpu.VMEM((N, N), F32)],
    )(twist, exchange(lines), high, low)
    return jnp.transpose(result, (1, 0, 2))


def solution(mesh):
    devices = mesh.devices.reshape(REP, 2, RING, 2, 2, 4)
    split = Mesh(devices, ("rep", "xh", "zh", "zl", "xl", "y"))
    row, col = ("xh", "zh", "zl"), ("xl", "y")
    return jax.shard_map(
        body,
        mesh=split,
        in_specs=(P("rep", col, row, None),),
        out_specs=P(("rep", *col), row, None),
        check_vma=False,
    )
```

```python
import ml_dtypes
import numpy as np

import jax
import jax.numpy as jnp
from jax import lax
from jax.experimental import pallas as pl
from jax.experimental.pallas import tpu as pltpu
from jax.sharding import Mesh
from jax.sharding import PartitionSpec as P

N = 384
SHIFT = 0.001
REP, COL, ROW = 2, 8, 32
GROUP = REP * COL
BLOCK = N // GROUP
CELLS = N // ROW
LINES = CELLS * BLOCK
TILES = BLOCK // 8
PACKED = 2 * TILES + 1
PARTS, PAIR = 4, 2
RING = ROW // PARTS
ORDER = (4, 0, 1, 5, 6, 2, 3, 7)
VMEM_BYTES = 12 * 2**20
F32 = jnp.float32
BF16 = jnp.bfloat16


def member_at(rep, col):
    return col % 4 * 4 + rep * 2 + col // 4


def block_of(member):
    rep, col = member // 2 % 2, member % 2 * 4 + member // 4
    return col * REP + rep


def tables():
    order = [
        BLOCK * block_of(member) + 8 * tile + low
        for tile in range(TILES)
        for member in range(GROUP)
        for low in range(8)
    ]
    turns = np.outer(np.asarray(order), np.arange(N)) % N
    angle = turns * (2.0 * np.pi / N)
    cas = np.cos(angle) + np.sin(angle)
    high = cas.astype(ml_dtypes.bfloat16)
    low = (cas - high.astype(np.float64)).astype(ml_dtypes.bfloat16)
    return high, low


def eigen_line():
    return (4.0 * np.sin(np.pi * np.arange(N) / N) ** 2).astype(np.float32)


def third_eigen():
    rows = [
        [
            BLOCK * block_of(member) + 8 * tile + PAIR * part + low
            for tile in range(TILES)
            for _ in range(PARTS)
            for low in range(PAIR)
        ]
        for member in range(GROUP)
        for part in range(PARTS)
    ]
    return eigen_line()[np.asarray(rows)]


def halves(x):
    high = x.astype(BF16)
    return high, (x - high.astype(F32)).astype(BF16)


def product(first, second, contract):
    dims = (contract, ((), ()))
    (fh, fl), (sh, sl) = first, second
    out = lax.dot_general(fl, sh, dims, preferred_element_type=F32)
    out += lax.dot_general(fh, sl, dims, preferred_element_type=F32)
    return out + lax.dot_general(fh, sh, dims, preferred_element_type=F32)


def lanes(shape):
    return lax.broadcasted_iota(jnp.int32, shape, 1)


def swapped(parts, width):
    parts = list(parts)
    lane = lanes(parts[0].shape)
    bit = 1
    while bit < len(parts):
        reach = width * bit
        upper = (lane & reach) != 0
        for i in range(len(parts)):
            if i & bit:
                continue
            a, b = parts[i], parts[i | bit]
            parts[i] = jnp.where(upper, pltpu.roll(b, reach, 1), a)
            parts[i | bit] = jnp.where(upper, b, pltpu.roll(a, 128 - reach, 1))
        bit *= 2
    return parts


def ratio_of(lam):
    root = jnp.sqrt(lam * (lam + 4.0))
    return 2.0 / (2.0 + lam + root), root


def send_tile(out_ref, member, piece, tile, twist=0):
    for part in range(PARTS):
        slot = GROUP * (part ^ twist) + member
        out_ref[slot, piece] = tile[PAIR * part : PAIR * (part + 1), :]


def received(in_ref, member, twist=0):
    parts = [in_ref[GROUP * (part ^ twist) + member] for part in range(PARTS)]
    return jnp.concatenate(parts, 1).reshape(8 * PACKED, 128)


def unit_place(unit, tile):
    if unit < 32:
        return unit % 16, 8 * (2 * tile + unit // 16)
    return 4 * tile + unit - 32, 8 * (PACKED - 1)


def first_kernel(twist_ref, mine_ref, got_ref, high_ref, low_ref, out_ref):
    density = (mine_ref[...] + got_ref[...]).reshape(LINES, N)
    pad = jnp.zeros((N - LINES, N), BF16)
    lines = tuple(jnp.concatenate([part, pad], 0) for part in halves(density))
    modes = product((high_ref[...], low_ref[...]), lines, ((1,), (1,)))
    rows = 8 * GROUP
    lane = lanes((rows, 128))
    rest = modes[0:rows, 256:384]
    for tile in range(1, TILES):
        moved = pltpu.roll(modes[rows * tile : rows * (tile + 1), 256:384], 32 * tile, 1)
        rest = jnp.where(lane < 32 * tile, rest, moved)
    for member in range(GROUP):
        at = 8 * member
        for tile in range(TILES):
            row = rows * tile + at
            for half in range(2):
                piece = modes[row : row + 8, 128 * half : 128 * half + 128]
                send_tile(out_ref, member, 2 * tile + half, piece, twist_ref[0])
        send_tile(out_ref, member, PACKED - 1, rest[at : at + 8], twist_ref[0])


def second_kernel(
    in_ref, lam_ref, high_ref, low_ref, field_ref, right_ref, left_ref, waves_ref, lines_ref
):
    packed = swapped([received(in_ref, member) for member in range(GROUP)], 8)
    for unit in range(CELLS * TILES):
        cell, piece = unit // TILES, unit % TILES
        for tile in range(TILES):
            source, at = unit_place(unit, tile)
            to = BLOCK * cell + 8 * tile
            lanes_to = slice(128 * piece, 128 * piece + 128)
            lines_ref[to : to + 8, lanes_to] = packed[source][at : at + 8]
    table = (high_ref[...], low_ref[...])
    field_ref[...] = product(halves(lines_ref[...]), table, ((1,), (0,)))
    ratio, _ = ratio_of(lam_ref[...])
    right = field_ref[0:BLOCK, :]
    left = field_ref[LINES - BLOCK : LINES, :]
    for i in range(1, CELLS):
        right = right * ratio + field_ref[BLOCK * i : BLOCK * (i + 1), :]
        j = CELLS - 1 - i
        left = left * ratio + field_ref[BLOCK * j : BLOCK * (j + 1), :]
    right_ref[...] = right
    left_ref[...] = left
    step = chunk_step(ratio)
    lower = sublanes((8, N)) < 4
    for tile in range(TILES):
        at = slice(8 * tile, 8 * tile + 8)
        joined = jnp.where(
            lower,
            step[at] * right[at] + pltpu.roll(right[at], 4, 0),
            step[at] * left[at] + pltpu.roll(left[at], 4, 0),
        )
        for member in range(RING):
            waves_ref[member, at, :] = joined


def chunk_step(ratio):
    square = ratio * ratio
    fourth = square * square
    return fourth * fourth * fourth


def sublanes(shape):
    return lax.broadcasted_iota(jnp.int32, shape, 0)


def ring_inflow(place, waves_ref, at, step):
    pair = step * step
    zero = jnp.zeros((8, N), F32)
    sides = []
    for forward in (True, False):
        before, rest, whole, decay = zero, zero, zero, jnp.ones((8, N), F32)
        for k in range(RING):
            member = k if forward else RING - 1 - k
            wave = waves_ref[ORDER.index(member), at, :]
            earlier = member < place if forward else member > place
            before = jnp.where(earlier, before * pair + wave, before)
            rest = jnp.where(earlier, rest, rest * pair + wave)
            whole = whole * pair + wave
            decay = jnp.where(earlier, decay * pair, decay)
        sides.append((before, rest, whole, decay))
    row = sublanes((8, N))
    before, rest, whole, decay = (jnp.where(row < 4, *both) for both in zip(*sides))
    first_arc = (row & 2) == 0
    other = jnp.where(first_arc, pltpu.roll(whole, 6, 0), pltpu.roll(whole, 2, 0))
    power = pair
    for _ in range(3):
        power = power * power
    return (before + decay * (other + power * rest)) / (1.0 - power * power)


def third_kernel(
    place_ref,
    field_ref,
    right_ref,
    left_ref,
    waves_ref,
    lam_ref,
    high_ref,
    low_ref,
    out_ref,
    lines_ref,
):
    ratio, root = ratio_of(lam_ref[...])
    step = chunk_step(ratio)
    lower = sublanes((8, N)) < 4
    forward, backward = [], []
    for tile in range(TILES):
        at = slice(8 * tile, 8 * tile + 8)
        inflow = ring_inflow(place_ref[0], waves_ref, at, step[at])
        turned = pltpu.roll(inflow, 4, 0)
        right = pltpu.roll(right_ref[at, :], 4, 0)
        left = pltpu.roll(left_ref[at, :], 4, 0)
        forward.append(jnp.where(lower, inflow, step[at] * turned + right))
        backward.append(jnp.where(lower, step[at] * turned + left, inflow))
    scale = (1.0 / (N * N)) / root
    run = jnp.concatenate(forward, 0)
    for i in range(CELLS):
        run = run * ratio
        lines_ref[BLOCK * i : BLOCK * (i + 1), :] = run
        run = run + field_ref[BLOCK * i : BLOCK * (i + 1), :]
    run = jnp.concatenate(backward, 0)
    for i in range(CELLS - 1, -1, -1):
        at = slice(BLOCK * i, BLOCK * (i + 1))
        run = run * ratio + field_ref[at, :]
        lines_ref[at, :] = (lines_ref[at, :] + run) * scale
    table = (high_ref[...], low_ref[...])
    lines_ref[...] = product(halves(lines_ref[...]), table, ((1,), (1,)))
    tiles = [[jnp.zeros((8, 128), F32)] * PACKED for _ in range(GROUP)]
    for unit in range(CELLS * TILES):
        cell, piece = unit // TILES, unit % TILES
        for tile in range(TILES):
            source, at = unit_place(unit, tile)
            row = BLOCK * cell + 8 * tile
            tiles[source][at // 8] = lines_ref[row : row + 8, 128 * piece : 128 * piece + 128]
    packed = swapped([jnp.concatenate(group, 0) for group in tiles], 8)
    for member in range(GROUP):
        slot = member_at(*divmod(block_of(member), COL))
        for piece in range(PACKED):
            send_tile(out_ref, slot, piece, packed[member][8 * piece : 8 * piece + 8])


def last_kernel(twist_ref, in_ref, high_ref, low_ref, out_ref, modes_ref):
    for member in range(GROUP):
        packed = received(in_ref, member, twist_ref[0])
        rest = packed[8 * (PACKED - 1) : 8 * PACKED]
        for tile in range(TILES):
            row = 8 * (GROUP * tile + member)
            for half in range(2):
                at = 8 * (2 * tile + half)
                modes_ref[row : row + 8, 128 * half : 128 * half + 128] = packed[at : at + 8]
            moved = rest if tile == 0 else pltpu.roll(rest, 128 - 32 * tile, 1)
            modes_ref[row : row + 8, 256:384] = moved
    table = (high_ref[...], low_ref[...])
    result = product(halves(modes_ref[...].T[0:LINES]), table, ((1,), (0,)))
    out_ref[...] = result.reshape(CELLS, BLOCK, N)


def call(kernel, name, **kwargs):
    params = pltpu.CompilerParams(vmem_limit_bytes=VMEM_BYTES)
    return pl.pallas_call(kernel, name=name, compiler_params=params, **kwargs)


def shaped(*shape):
    return jax.ShapeDtypeStruct(shape, F32)


def lines_scratch():
    return pltpu.VMEM((LINES, N), F32)


def copy_kernel(rep_ref, in_ref, out_ref):
    out_ref[...] = in_ref[...]


def own_half(part, rep):
    shape = (CELLS, BLOCK, N)
    grid_spec = pltpu.PrefetchScalarGridSpec(
        num_scalar_prefetch=1,
        grid=(1,),
        in_specs=[pl.BlockSpec(shape, lambda i, rep_ref: (0, rep_ref[0], 0))],
        out_specs=pl.BlockSpec(shape, lambda i, rep_ref: (0, 0, 0)),
    )
    out = shaped(*shape)
    return call(copy_kernel, "mine", grid_spec=grid_spec, out_shape=out)(rep.reshape(1), part)


def exchange(x):
    return lax.all_to_all(x, ("zl", "xh", "y", "rep", "xl"), 0, 0, tiled=True)


def ring_exchange(x):
    rings = [[2 * k + (half ^ (k // (RING // 2))) for k in ORDER] for half in range(2)]
    return lax.all_to_all(x, ("zh", "zl"), 0, 0, axis_index_groups=rings, tiled=True)


def body(sources):
    rep, col = lax.axis_index("rep"), lax.axis_index("xl") * 4 + lax.axis_index("y")
    place = lax.axis_index("zh")
    twist = 2 * (place // (RING // 2))
    part_index = (lax.axis_index("zl") * 2 + lax.axis_index("xh")) ^ twist
    high, low = (jnp.asarray(part) for part in tables())
    part = jnp.transpose(sources[0], (1, 0, 2))
    mine = own_half(part, rep)
    other = lax.dynamic_slice_in_dim(part, (1 - rep) * BLOCK, BLOCK, 1)
    got = lax.ppermute(other, "rep", [(0, 1), (1, 0)])
    eigen = jnp.asarray(eigen_line())
    third = jnp.asarray(third_eigen())
    third = lax.dynamic_index_in_dim(third, member_at(rep, col) * PARTS + part_index, keepdims=False)
    lam = third[:, None] + eigen[None, :] + SHIFT
    packed = shaped(GROUP * PARTS, PACKED, PAIR, 128)
    vmem = pl.BlockSpec(memory_space=pltpu.VMEM)
    smem = pl.BlockSpec(memory_space=pltpu.SMEM)
    place, twist = place.reshape(1), twist.reshape(1)
    modes = call(first_kernel, "first", in_specs=[smem] + [vmem] * 4, out_shape=packed)(
        twist, mine, got, high, low
    )
    modes, lam, place, twist = lax.optimization_barrier((modes, lam, place, twist))
    side = shaped(BLOCK, N)
    field, right, left, waves = call(
        second_kernel,
        "second",
        out_shape=(shaped(LINES, N), side, side, shaped(RING, BLOCK, N)),
        scratch_shapes=[lines_scratch()],
    )(exchange(modes), lam, high, low)
    waves = ring_exchange(waves)
    lines = call(
        third_kernel,
        "third",
        in_specs=[smem] + [vmem] * 7,
        out_shape=packed,
        scratch_shapes=[lines_scratch()],
    )(place, field, right, left, waves, lam, high, low)
    result = call(
        last_kernel,
        "last",
        in_specs=[smem] + [vmem] * 3,
        out_shape=shaped(CELLS, BLOCK, N),
        scratch_shapes=[pltpu.VMEM((N, N), F32)],
    )(twist, exchange(lines), high, low)
    return jnp.transpose(result, (1, 0, 2))


def solution(mesh):
    devices = mesh.devices.reshape(REP, 2, RING, 2, 2, 4)
    split = Mesh(devices, ("rep", "xh", "zh", "zl", "xl", "y"))
    row, col = ("xh", "zh", "zl"), ("xl", "y")
    return jax.shard_map(
        body,
        mesh=split,
        in_specs=(P("rep", col, row, None),),
        out_specs=P(("rep", *col), row, None),
        check_vma=False,
    )
```
